32 devices in a mesh: row: 4 (over z), col: 4 (over x, core), depth: 2 (over y).
Axes of the slice: x: 2, y: 2, z: 4, core: 2. Of those that a mesh axis runs over, the one named last changes fastest.
Arguments:
- tokens: bfloat16 [2048, 8192], P(('row', 'col'), 'depth'), may hold values from -0.3125 to 0.3125
- weight: bfloat16 [8192, 8192], P('depth', ('col', 'row')), may hold values from -0.0625 to 0.0625
- grad_output: bfloat16 [2048, 8192], P('row', ('col', 'depth')), may hold values from -6 to 6
Outputs:
- grad_input: bfloat16 [2048, 8192], P(('row', 'col'), 'depth')
- grad_weight: bfloat16 [8192, 8192], P('depth', ('col', 'row'))
The draws below stay inside these ranges and needn't reach their ends.
All inputs are finite; a program needn't handle non-finite values.
Results may differ from the reference program's by a relative error of at most 0.001.
Values may be sent and summed in bfloat16 or wider, within the bound.
A program may use at most 128 MiB of HBM per device.

```python
import jax
import jax.numpy as jnp

D_IN = 8192
D_OUT = 8192
TOKENS = 2048


def spiked(drawn, stream_key, source, target, parts, factor):
    def block_of(axis_at):
        return (jnp.arange(drawn.shape[axis_at]) // (drawn.shape[axis_at] // parts)).reshape((-1,) + (1,) * (drawn.ndim - 1 - axis_at))

    one_side = jax.random.permutation(stream_key, parts)[block_of(target)]
    other_side = (block_of(target) + parts // 2) % parts
    return jnp.where((block_of(source) == one_side) | (block_of(source) == other_side), factor * drawn, drawn)


def shard_levels(rng, extent, pieces, low, top_value):
    gain, own = 1.0, jax.random.fold_in(rng, 6)
    for position, shards_of in pieces:
        steps = jnp.exp(jax.random.uniform(jax.random.fold_in(own, position), (shards_of,), jnp.float32, low / len(pieces), top_value / len(pieces)))
        gain = gain * jnp.repeat(steps, extent[position] // shards_of).reshape([-1 if axis == position else 1 for axis in range(len(extent))])
    return gain


def bell_draw(rng, dims, width, reach, pieces=(), kind=jnp.bfloat16):
    factor_of = shard_levels(rng, dims, pieces, -0.22, 0.18) if pieces else 1.0
    result = jax.random.normal(rng, dims, jnp.float32) * width * factor_of
    return jnp.minimum(jnp.maximum(result, -reach), reach).astype(kind)


def bell_draw_with(stream_key, shape, width, most, pieces, heavy, held_as=jnp.bfloat16):
    drawn = width * jax.random.normal(stream_key, shape, jnp.float32)
    if pieces:
        drawn = drawn * shard_levels(stream_key, shape, pieces, -0.22, 0.18)
    return jnp.clip(spiked(drawn, jax.random.fold_in(stream_key, 3), *heavy), -most, most).astype(held_as)


def setup_inputs(seed: int = 0) -> dict:
    keys = jax.random.split(jax.random.key(seed), 4)
    tokens = bell_draw(keys[0], (TOKENS, D_IN), (TOKENS ** -0.5), 0.3125, ((0, 16), (1, 2)))
    weight = bell_draw(keys[1], (D_IN, D_OUT), D_IN ** -0.5, 0.0625, ((0, 2), (1, 16)))
    grad_output = bell_draw_with(keys[2], (TOKENS, D_OUT), 1.0, 6.0, ((0, 4), (1, 8)), (1, 0, 8, 2.0))
    return {"tokens": tokens, "weight": weight, "grad_output": grad_output}


def reference(tokens, weight, grad_output):
    grad_input = jnp.dot(grad_output, weight.T, preferred_element_type=jnp.float32).astype(jnp.bfloat16)
    grad_weight = jnp.dot(tokens.T, grad_output, preferred_element_type=jnp.float32).astype(jnp.bfloat16)
    return grad_input, grad_weight
```

```python
import jax
import jax.numpy as jnp
from jax import lax
from jax.experimental import pallas as pl
from jax.experimental.pallas import tpu as pltpu
from jax.sharding import PartitionSpec as P

last_with_last = (((1,), (1,)), ((), ()))
first_with_first = (((0,), (0,)), ((), ()))
MESH = pl.DeviceIdType.MESH
CHUNKS = 4
GROUP = 16
SPAN = 83.0
TINY = 1e-30
F32, BF16 = jnp.float32, jnp.bfloat16


def input_grads(weight, grad_block):
    weight_block = lax.all_gather(weight, "row", axis=1, tiled=True)
    partial_value = lax.dot_general(
        grad_block, weight_block, last_with_last, preferred_element_type=jnp.float32
    )
    column_slab = lax.psum_scatter(partial_value, "col", scatter_dimension=1, tiled=True).astype(
        jnp.bfloat16
    )
    return lax.all_to_all(column_slab, "col", split_axis=0, concat_axis=1, tiled=True)


def weight_grads(tokens, grad_block):
    partial_value = lax.dot_general(
        lax.all_gather(tokens, "col", axis=0, tiled=True),
        grad_block,
        first_with_first,
        preferred_element_type=jnp.float32,
    )
    return lax.psum_scatter(partial_value, "row", scatter_dimension=1, tiled=True).astype(
        jnp.bfloat16
    )


def per_device_general(tokens, weight, grad_output):
    grad_block = lax.all_gather(grad_output, "depth", axis=1, tiled=True)
    grad_input = input_grads(weight, grad_block)
    grad_weight = weight_grads(tokens, grad_block)
    return (grad_input, grad_weight)


def place(c):
    return 2 * (c % 2) + c // 2


def kernel(
    tok, w, g, gi, gw,
    g_all, g_mid, x_all, x_t, w_all, part, gw_out, gi_out, ups, upr, dns, dnr,
    g_pre, g_z, g_x, g_y, g_d, x_r, w_r, x_z, up_r, dn_r, gi_r, gw_r,
    s_pre, s_z, s_x, s_y, s_d, s_xc, s_w, s_xz, s_up, s_dn, s_gi, s_gw, l_gi, l_gw,
):
    r, c, d = lax.axis_index("row"), lax.axis_index("col"), lax.axis_index("depth")
    k, x = c % 2, c // 2
    other = 1 - d
    core = c + 1 - 2 * k
    across = c + 2 - 4 * x
    diagonal = 3 - c
    peers = (across, diagonal, core)
    tl, il = tok.shape
    tb = 4 * tl
    half = tb // 2
    ib = il // 4
    ic = ib // CHUNKS
    ol = w.shape[1]

    barrier = pltpu.get_barrier_semaphore()
    for q in peers:
        pl.semaphore_signal(barrier, inc=1, device_id={"col": q}, device_id_type=MESH)
    pl.semaphore_signal(barrier, inc=1, device_id={"depth": other}, device_id_type=MESH)
    for s in (1, 2, 3):
        pl.semaphore_signal(barrier, inc=1, device_id={"row": (r + s) % 4}, device_id_type=MESH)
    pl.semaphore_wait(barrier, 7)

    sent = []

    def when(cond, f):
        if cond is None:
            f()
        else:
            pl.when(cond)(f)

    def send(src, dst, s_sem, r_sem, to, cond=None):
        copy = pltpu.make_async_remote_copy(
            src_ref=src, dst_ref=dst, send_sem=s_sem, recv_sem=r_sem, device_id=to, device_id_type=MESH
        )
        when(cond, copy.start)
        sent.append((copy.wait_send, cond))

    def local(src, dst, sem, cond=None):
        when(cond, pltpu.make_async_copy(src, dst, sem).start)

    def arrived(ref, sem, cond=None):
        when(cond, pltpu.make_async_copy(ref, ref, sem).wait)

    def at(i, n):
        return pl.ds(pl.multiple_of(i * n, n), n)

    def g_unit(s, h, q):
        return g_all.at[at(s * 2 + h, half), at(place(q), ol)]

    for h in (0, 1):
        to = 2 * d + h
        mine = to == r
        ours = g.at[at(d, half), at(h, ol)]
        theirs = g.at[at(other, half), at(h, ol)]
        send(theirs, g_unit(r, other, c), s_pre.at[h], g_z.at[r], {"depth": other}, mine)
        send(theirs, g_mid.at[h], s_pre.at[h], g_pre.at[h], {"depth": other}, jnp.logical_not(mine))
        local(ours, g_unit(r, d, c), g_z.at[r], mine)
        send(ours, g_unit(r, d, c), s_z.at[h], g_z.at[r], {"row": to}, jnp.logical_not(mine))

    def send_tokens(j):
        for i, q in enumerate(peers):
            send(
                tok.at[:, at(q * CHUNKS + j, ic)], x_all.at[j, at(r * 4 + c, tl)],
                s_xc.at[j, i], x_r.at[j, c], {"col": q},
            )
        local(tok.at[:, at(c * CHUNKS + j, ic)], x_all.at[j, at(r * 4 + c, tl)], x_r.at[j, c])

    def send_weight(j):
        for i, q in enumerate(peers):
            send(
                w.at[at(q * CHUNKS + j, ic)], w_all.at[j, :, at(place(c), ol)],
                s_w.at[j, i], w_r.at[j, c], {"col": q},
            )
        local(w.at[at(c * CHUNKS + j, ic)], w_all.at[j, :, at(place(c), ol)], w_r.at[j, c])

    for j in range(CHUNKS):
        send_tokens(j)
    send_weight(0)

    def tokens_on(j, s, direction, cond):
        block = x_all.at[j, at(s, tb)]
        send(block, block, s_xz.at[j, direction, s], x_z.at[j, s], {"row": r + 1 - 2 * direction}, cond)

    up_ok, down_ok = r < 3, r > 0

    def own_tokens_on(j):
        for q in range(4):
            arrived(x_all.at[j, at(r * 4 + q, tl)], x_r.at[j, q])
        tokens_on(j, r, 0, up_ok)
        tokens_on(j, r, 1, down_ok)

    def pass_tokens(j, far):
        below, above = r - far, r + far
        low, high = jnp.maximum(below, 0), jnp.minimum(above, 3)
        has_low, has_high = below >= 0, above <= 3
        arrived(x_all.at[j, at(low, tb)], x_z.at[j, low], has_low)
        tokens_on(j, low, 0, jnp.logical_and(has_low, up_ok))
        arrived(x_all.at[j, at(high, tb)], x_z.at[j, high], has_high)
        tokens_on(j, high, 1, jnp.logical_and(has_high, down_ok))

    order = [(r, None)]
    for far in (1, 2, 3):
        order.append((jnp.maximum(r - far, 0), r - far >= 0))
        order.append((jnp.minimum(r + far, 3), r + far <= 3))

    def spread(s, cond):
        unit = g_unit(s, d, c)
        arrived(unit, g_z.at[s], cond)
        send(unit, unit, s_x.at[s], g_x.at[s], {"col": across}, cond)
        send(unit, unit, s_y.at[0, s], g_y.at[0, s], {"depth": other}, cond)

    def spread_crossed(s, cond):
        unit = g_unit(s, d, across)
        arrived(unit, g_x.at[s], cond)
        send(unit, unit, s_y.at[1, s], g_y.at[1, s], {"depth": other}, cond)

    def to_core(s, cond):
        arrived(g_unit(s, other, c), g_y.at[0, s], cond)
        arrived(g_unit(s, other, across), g_y.at[1, s], cond)
        slab = g_all.at[at(s, tb), at(k, 2 * ol)]
        send(slab, slab, s_d.at[s], g_d.at[s], {"col": core}, cond)

    own_tokens_on(0)
    own_tokens_on(1)
    for h in (0, 1):
        to = 2 * other + h
        go = to != r
        arrived(g_mid.at[h], g_pre.at[h], go)
        send(g_mid.at[h], g_unit(r, d, c), s_z.at[2 + h], g_z.at[r], {"row": to}, go)
    spread(*order[0])
    own_tokens_on(2)
    own_tokens_on(3)
    spread(*order[1])
    spread(*order[2])
    pass_tokens(0, 1)
    spread(*order[3])
    spread(*order[4])
    pass_tokens(1, 1)
    spread(*order[5])
    spread(*order[6])
    for j in range(1, CHUNKS):
        send_weight(j)
    pass_tokens(2, 1)
    pass_tokens(3, 1)
    for n, (s, cond) in enumerate(order):
        spread_crossed(s, cond)
        if n >= 3:
            pass_tokens(n - 3, 2)
    for s, cond in order:
        to_core(s, cond)
    for s in range(4):
        arrived(g_all.at[at(s, tb), at(1 - k, 2 * ol)], g_d.at[s])

    def multiply_input(j):
        for q in range(4):
            arrived(w_all.at[j, :, at(place(q), ol)], w_r.at[j, q])

        def body(b, carry):
            rows = at(b, tb)
            part[j, rows, :] = lax.dot_general(
                g_all[rows, :], w_all[j], last_with_last, preferred_element_type=F32
            )
            return carry

        lax.fori_loop(0, 4, body, None)

    def multiply_weight(j):
        def turn(b, carry):
            x_t[:, at(b, half)] = x_all[j, at(b, half), :].T
            return carry

        lax.fori_loop(0, 8, turn, None)

        def body(n, carry):
            cols = at(n, ol)
            gw_out[j, :, cols] = jnp.dot(
                x_t[...], g_all[:, cols], preferred_element_type=F32
            ).astype(BF16)
            return carry

        lax.fori_loop(0, 4, body, None)
        for i, q in enumerate(peers):
            send(
                gw_out.at[j, :, at(place(q), ol)], gw.at[at(c * CHUNKS + j, ic)],
                s_gw.at[j, i], gw_r.at[j, c], {"col": q},
            )
        local(gw_out.at[j, :, at(place(c), ol)], gw.at[at(c * CHUNKS + j, ic)], l_gw.at[j])

    step = 64
    scale_rows = pl.ds(tb, GROUP)

    def read_code(buf, i, rows, unit):
        v = buf[i, rows, :].astype(F32)
        size = jnp.log(jnp.abs(v)) + SPAN
        size = size * jnp.concatenate([unit] * (step // GROUP), axis=0)
        return jnp.where(v < 0, -size, size)

    def unit_of(buf, i):
        return buf[i, scale_rows, :].astype(F32) * (0.5 / SPAN)

    def encode(j, b, out, slot, got):
        unit = None if got is None else unit_of(got, slot)

        def total(t):
            value = part[j, pl.ds(pl.multiple_of(b * tb + t * step, step), step), :]
            if got is not None:
                value = value + read_code(got, slot, at(t, step), unit)
            return value

        def first(t, most):
            value = total(t)
            if got is not None:
                part[j, pl.ds(pl.multiple_of(b * tb + t * step, step), step), :] = value
            size = jnp.abs(value)
            for n in range(step // GROUP):
                most = jnp.maximum(most, size[n * GROUP : (n + 1) * GROUP])
            return most

        most = lax.fori_loop(0, tb // step, first, jnp.full((GROUP, ic), TINY, F32))
        scale = (most * 1.01).astype(BF16)
        out[slot, scale_rows, :] = scale
        by = (2 * SPAN) / scale.astype(F32)
        by = jnp.concatenate([by] * (step // GROUP), axis=0)

        def second(t, carry):
            value = part[j, pl.ds(pl.multiple_of(b * tb + t * step, step), step), :]
            code = jnp.exp(jnp.abs(value) * by - SPAN)
            out[slot, at(t, step), :] = jnp.where(value < 0, -code, code).astype(BF16)
            return carry

        lax.fori_loop(0, tb // step, second, None)

    def add_in(j, got, slot):
        unit = unit_of(got, slot)

        def body(t, carry):
            rows = pl.ds(pl.multiple_of(r * tb + t * step, step), step)
            part[j, rows, :] = part[j, rows, :] + read_code(got, slot, at(t, step), unit)
            return carry

        lax.fori_loop(0, tb // step, body, None)

    def ring(j, level, up):
        here = level if up else 3 - level
        out, got, s_sem, r_sem = (ups, upr, s_up, up_r) if up else (dns, dnr, s_dn, dn_r)
        toward = {"row": r + 1 if up else r - 1}
        far = [3, 2, 1, 0] if up else [0, 1, 2, 3]

        def slot_of(b):
            return j * 3 + (b - 1 if up else b)

        copies = []
        for b in far[: 3 - level]:
            i = slot_of(b)
            copies.append(
                (b, i, pltpu.make_async_remote_copy(
                    src_ref=out.at[i], dst_ref=got.at[i], send_sem=s_sem.at[i], recv_sem=r_sem.at[i],
                    device_id=toward, device_id_type=MESH,
                ))
            )
        cond = r == here

        @pl.when(cond)
        def _():
            for b, i, copy in copies:
                if level > 0:
                    arrived(got.at[i], r_sem.at[i])
                encode(j, b, out, i, got if level > 0 else None)
                copy.start()
            if level > 0:
                i = slot_of(here)
                arrived(got.at[i], r_sem.at[i])
                add_in(j, got, i)

        for _, _, copy in copies:
            sent.append((copy.wait_send, cond))

    def level(j, n):
        ring(j, n, True)
        ring(j, n, False)

    def finish(j, cond):
        @pl.when(cond)
        def _():
            gi_out[j] = part[j, at(r, tb), :].astype(BF16)

        for i, q in enumerate(peers):
            send(
                gi_out.at[j, at(q, tl)], gi.at[:, at(c * CHUNKS + j, ic)],
                s_gi.at[j, i], gi_r.at[j, c], {"col": q}, cond,
            )
        local(gi_out.at[j, at(c, tl)], gi.at[:, at(c * CHUNKS + j, ic)], l_gi.at[j], cond)

    inner = jnp.logical_or(r == 1, r == 2)
    outer = jnp.logical_or(r == 0, r == 3)

    multiply_input(0)
    level(0, 0)
    multiply_input(1)
    level(1, 0)
    level(0, 1)
    pass_tokens(0, 3)
    multiply_weight(0)
    multiply_input(2)
    level(2, 0)
    level(1, 1)
    level(0, 2)
    finish(0, inner)
    pass_tokens(1, 3)
    multiply_weight(1)
    multiply_input(3)
    level(3, 0)
    level(2, 1)
    level(1, 2)
    finish(1, inner)
    level(0, 3)
    finish(0, outer)
    pass_tokens(2, 3)
    multiply_weight(2)
    level(3, 1)
    level(2, 2)
    finish(2, inner)
    level(1, 3)
    finish(1, outer)
    pass_tokens(3, 3)
    multiply_weight(3)
    level(3, 2)
    finish(3, inner)
    level(2, 3)
    finish(2, outer)
    level(3, 3)
    finish(3, outer)

    for wait, cond in sent:
        when(cond, wait)
    for j in range(CHUNKS):
        arrived(gi.at[:, at(c * CHUNKS + j, ic)], l_gi.at[j])
        arrived(gw.at[at(c * CHUNKS + j, ic)], l_gw.at[j])
        for q in peers:
            arrived(gi.at[:, at(q * CHUNKS + j, ic)], gi_r.at[j, q])
            arrived(gw.at[at(q * CHUNKS + j, ic)], gw_r.at[j, q])


def per_device_kernel(tokens, weight, grad_output):
    tl, il = tokens.shape
    ol = weight.shape[1]
    tb, ic = 4 * tl, il // (4 * CHUNKS)
    dma = pltpu.SemaphoreType.DMA
    code = pltpu.VMEM((3 * CHUNKS, tb + GROUP, ic), BF16)
    anywhere = pl.BlockSpec(memory_space=pl.ANY)
    return pl.pallas_call(
        kernel,
        out_shape=(
            jax.ShapeDtypeStruct(tokens.shape, BF16),
            jax.ShapeDtypeStruct(weight.shape, BF16),
        ),
        in_specs=[anywhere] * 3,
        out_specs=(anywhere, anywhere),
        scratch_shapes=[
            pltpu.VMEM((4 * tb, 4 * ol), BF16),
            pltpu.VMEM((2, tb // 2, ol), BF16),
            pltpu.VMEM((CHUNKS, 4 * tb, ic), BF16),
            pltpu.VMEM((ic, 4 * tb), BF16),
            pltpu.VMEM((CHUNKS, ic, 4 * ol), BF16),
            pltpu.VMEM((CHUNKS, 4 * tb, ic), F32),
            pltpu.VMEM((CHUNKS, ic, 4 * ol), BF16),
            pltpu.VMEM((CHUNKS, tb, ic), BF16),
            code, code, code, code,
            dma((2,)), dma((4,)), dma((4,)), dma((2, 4)), dma((4,)),
            dma((CHUNKS, 4)), dma((CHUNKS, 4)), dma((CHUNKS, 4)),
            dma((3 * CHUNKS,)), dma((3 * CHUNKS,)), dma((CHUNKS, 4)), dma((CHUNKS, 4)),
            dma((2,)), dma((4,)), dma((4,)), dma((2, 4)), dma((4,)),
            dma((CHUNKS, 3)), dma((CHUNKS, 3)), dma((CHUNKS, 2, 4)),
            dma((3 * CHUNKS,)), dma((3 * CHUNKS,)), dma((CHUNKS, 3)), dma((CHUNKS, 3)),
            dma((CHUNKS,)), dma((CHUNKS,)),
        ],
        compiler_params=pltpu.CompilerParams(
            collective_id=0, has_side_effects=True, vmem_limit_bytes=62 * 2**20
        ),
    )(tokens, weight, grad_output)


def solution(mesh):
    fours_fit = mesh.shape["row"] == 4 and mesh.shape["col"] == 4 and mesh.shape["depth"] == 2
    return jax.shard_map(
        per_device_kernel if fours_fit else per_device_general,
        mesh=mesh,
        in_specs=(
            P(("row", "col"), "depth"),
            P("depth", ("col", "row")),
            P("row", ("col", "depth")),
        ),
        out_specs=(P(("row", "col"), "depth"), P("depth", ("col", "row"))),
        check_vma=False,
    )
```

```python
import jax
import jax.numpy as jnp
from jax import lax
from jax.experimental import pallas as pl
from jax.experimental.pallas import tpu as pltpu
from jax.sharding import PartitionSpec as P

last_with_last = (((1,), (1,)), ((), ()))
first_with_first = (((0,), (0,)), ((), ()))
MESH = pl.DeviceIdType.MESH
CHUNKS = 4
GROUP = 16
SPAN = 83.0
TINY = 1e-30
F32, BF16 = jnp.float32, jnp.bfloat16


def input_grads(weight, grad_block):
    weight_block = lax.all_gather(weight, "row", axis=1, tiled=True)
    partial_value = lax.dot_general(
        grad_block, weight_block, last_with_last, preferred_element_type=jnp.float32
    )
    column_slab = lax.psum_scatter(partial_value, "col", scatter_dimension=1, tiled=True).astype(
        jnp.bfloat16
    )
    return lax.all_to_all(column_slab, "col", split_axis=0, concat_axis=1, tiled=True)


def weight_grads(tokens, grad_block):
    partial_value = lax.dot_general(
        lax.all_gather(tokens, "col", axis=0, tiled=True),
        grad_block,
        first_with_first,
        preferred_element_type=jnp.float32,
    )
    return lax.psum_scatter(partial_value, "row", scatter_dimension=1, tiled=True).astype(
        jnp.bfloat16
    )


def per_device_general(tokens, weight, grad_output):
    grad_block = lax.all_gather(grad_output, "depth", axis=1, tiled=True)
    grad_input = input_grads(weight, grad_block)
    grad_weight = weight_grads(tokens, grad_block)
    return (grad_input, grad_weight)


def place(c):
    return 2 * (c % 2) + c // 2


def kernel(
    tok, w, g, gi, gw,
    g_all, g_mid, x_all, x_t, w_all, part, gw_out, gi_out, ups, upr, dns, dnr,
    g_pre, g_z, g_x, g_y, g_d, x_r, w_r, x_z, up_r, dn_r, gi_r, gw_r,
    s_pre, s_z, s_x, s_y, s_d, s_xc, s_w, s_xz, s_up, s_dn, s_gi, s_gw, l_gi, l_gw,
):
    r, c, d = lax.axis_index("row"), lax.axis_index("col"), lax.axis_index("depth")
    k, x = c % 2, c // 2
    other = 1 - d
    core = c + 1 - 2 * k
    across = c + 2 - 4 * x
    diagonal = 3 - c
    peers = (across, diagonal, core)
    tl, il = tok.shape
    tb = 4 * tl
    half = tb // 2
    ib = il // 4
    ic = ib // CHUNKS
    ol = w.shape[1]

    barrier = pltpu.get_barrier_semaphore()
    for q in peers:
        pl.semaphore_signal(barrier, inc=1, device_id={"col": q}, device_id_type=MESH)
    pl.semaphore_signal(barrier, inc=1, device_id={"depth": other}, device_id_type=MESH)
    for s in (1, 2, 3):
        pl.semaphore_signal(barrier, inc=1, device_id={"row": (r + s) % 4}, device_id_type=MESH)
    pl.semaphore_wait(barrier, 7)

    sent = []

    def when(cond, f):
        if cond is None:
            f()
        else:
            pl.when(cond)(f)

    def send(src, dst, s_sem, r_sem, to, cond=None):
        copy = pltpu.make_async_remote_copy(
            src_ref=src, dst_ref=dst, send_sem=s_sem, recv_sem=r_sem, device_id=to, device_id_type=MESH
        )
        when(cond, copy.start)
        sent.append((copy.wait_send, cond))

    def local(src, dst, sem, cond=None):
        when(cond, pltpu.make_async_copy(src, dst, sem).start)

    def arrived(ref, sem, cond=None):
        when(cond, pltpu.make_async_copy(ref, ref, sem).wait)

    def at(i, n):
        return pl.ds(pl.multiple_of(i * n, n), n)

    def g_unit(s, h, q):
        return g_all.at[at(s * 2 + h, half), at(place(q), ol)]

    for h in (0, 1):
        to = 2 * d + h
        mine = to == r
        ours = g.at[at(d, half), at(h, ol)]
        theirs = g.at[at(other, half), at(h, ol)]
        send(theirs, g_unit(r, other, c), s_pre.at[h], g_z.at[r], {"depth": other}, mine)
        send(theirs, g_mid.at[h], s_pre.at[h], g_pre.at[h], {"depth": other}, jnp.logical_not(mine))
        local(ours, g_unit(r, d, c), g_z.at[r], mine)
        send(ours, g_unit(r, d, c), s_z.at[h], g_z.at[r], {"row": to}, jnp.logical_not(mine))

    def send_tokens(j):
        for i, q in enumerate(peers):
            send(
                tok.at[:, at(q * CHUNKS + j, ic)], x_all.at[j, at(r * 4 + c, tl)],
                s_xc.at[j, i], x_r.at[j, c], {"col": q},
            )
        local(tok.at[:, at(c * CHUNKS + j, ic)], x_all.at[j, at(r * 4 + c, tl)], x_r.at[j, c])

    def send_weight(j):
        for i, q in enumerate(peers):
            send(
                w.at[at(q * CHUNKS + j, ic)], w_all.at[j, :, at(place(c), ol)],
                s_w.at[j, i], w_r.at[j, c], {"col": q},
            )
        local(w.at[at(c * CHUNKS + j, ic)], w_all.at[j, :, at(place(c), ol)], w_r.at[j, c])

    for j in range(CHUNKS):
        send_tokens(j)
    send_weight(0)

    def tokens_on(j, s, direction, cond):
        block = x_all.at[j, at(s, tb)]
        send(block, block, s_xz.at[j, direction, s], x_z.at[j, s], {"row": r + 1 - 2 * direction}, cond)

    up_ok, down_ok = r < 3, r > 0

    def own_tokens_on(j):
        for q in range(4):
            arrived(x_all.at[j, at(r * 4 + q, tl)], x_r.at[j, q])
        tokens_on(j, r, 0, up_ok)
        tokens_on(j, r, 1, down_ok)

    def pass_tokens(j, far):
        below, above = r - far, r + far
        low, high = jnp.maximum(below, 0), jnp.minimum(above, 3)
        has_low, has_high = below >= 0, above <= 3
        arrived(x_all.at[j, at(low, tb)], x_z.at[j, low], has_low)
        tokens_on(j, low, 0, jnp.logical_and(has_low, up_ok))
        arrived(x_all.at[j, at(high, tb)], x_z.at[j, high], has_high)
        tokens_on(j, high, 1, jnp.logical_and(has_high, down_ok))

    near = 3 * (1 - r // 2)
    last = 1 + r % 2
    order = [near, 6 - r - near - last, last, r]

    def spread(n):
        s = order[n]
        unit = g_unit(s, d, c)
        arrived(unit, g_z.at[s])
        send(unit, unit, s_x.at[s], g_x.at[s], {"col": across})
        send(unit, unit, s_y.at[0, s], g_y.at[0, s], {"depth": other})

    def crossed(n):
        s = order[n]
        unit = g_unit(s, d, across)
        arrived(unit, g_x.at[s])
        send(unit, unit, s_y.at[1, s], g_y.at[1, s], {"depth": other})

    def to_core(n):
        s = order[n]
        arrived(g_unit(s, other, c), g_y.at[0, s])
        arrived(g_unit(s, other, across), g_y.at[1, s])
        slab = g_all.at[at(s, tb), at(k, 2 * ol)]
        send(slab, slab, s_d.at[s], g_d.at[s], {"col": core})

    def pass_mid(h):
        to = 2 * other + h
        go = to != r
        arrived(g_mid.at[h], g_pre.at[h], go)
        send(g_mid.at[h], g_unit(r, d, c), s_z.at[2 + h], g_z.at[r], {"row": to}, go)

    def from_core(n):
        s = order[n]
        arrived(g_all.at[at(s, tb), at(1 - k, 2 * ol)], g_d.at[s])

    def weight_in(j):
        for q in range(4):
            arrived(w_all.at[j, :, at(place(q), ol)], w_r.at[j, q])

    def multiply_block(j, s):
        rows = at(s, tb)
        part[j, rows, :] = lax.dot_general(
            g_all[rows, :], w_all[j], last_with_last, preferred_element_type=F32
        )

    def multiply_input(j):
        def body(b, carry):
            multiply_block(j, b)
            return carry

        lax.fori_loop(0, 4, body, None)

    def multiply_weight(j):
        def turn(b, carry):
            x_t[:, at(b, half)] = x_all[j, at(b, half), :].T
            return carry

        lax.fori_loop(0, 8, turn, None)

        def body(n, carry):
            cols = at(n, ol)
            gw_out[j, :, cols] = jnp.dot(
                x_t[...], g_all[:, cols], preferred_element_type=F32
            ).astype(BF16)
            return carry

        lax.fori_loop(0, 4, body, None)
        for i, q in enumerate(peers):
            send(
                gw_out.at[j, :, at(place(q), ol)], gw.at[at(c * CHUNKS + j, ic)],
                s_gw.at[j, i], gw_r.at[j, c], {"col": q},
            )
        local(gw_out.at[j, :, at(place(c), ol)], gw.at[at(c * CHUNKS + j, ic)], l_gw.at[j])

    step = 64
    scale_rows = pl.ds(tb, GROUP)

    def read_code(buf, i, rows, unit):
        v = buf[i, rows, :].astype(F32)
        size = jnp.log(jnp.abs(v)) + SPAN
        size = size * jnp.concatenate([unit] * (step // GROUP), axis=0)
        return jnp.where(v < 0, -size, size)

    def unit_of(buf, i):
        return buf[i, scale_rows, :].astype(F32) * (0.5 / SPAN)

    def encode(j, b, out, slot, got):
        unit = None if got is None else unit_of(got, slot)

        def total(t):
            value = part[j, pl.ds(pl.multiple_of(b * tb + t * step, step), step), :]
            if got is not None:
                value = value + read_code(got, slot, at(t, step), unit)
            return value

        def first(t, most):
            value = total(t)
            if got is not None:
                part[j, pl.ds(pl.multiple_of(b * tb + t * step, step), step), :] = value
            size = jnp.abs(value)
            for n in range(step // GROUP):
                most = jnp.maximum(most, size[n * GROUP : (n + 1) * GROUP])
            return most

        most = lax.fori_loop(0, tb // step, first, jnp.full((GROUP, ic), TINY, F32))
        scale = (most * 1.01).astype(BF16)
        out[slot, scale_rows, :] = scale
        by = (2 * SPAN) / scale.astype(F32)
        by = jnp.concatenate([by] * (step // GROUP), axis=0)

        def second(t, carry):
            value = part[j, pl.ds(pl.multiple_of(b * tb + t * step, step), step), :]
            code = jnp.exp(jnp.abs(value) * by - SPAN)
            out[slot, at(t, step), :] = jnp.where(value < 0, -code, code).astype(BF16)
            return carry

        lax.fori_loop(0, tb // step, second, None)

    def add_in(j, got, slot):
        unit = unit_of(got, slot)

        def body(t, carry):
            rows = pl.ds(pl.multiple_of(r * tb + t * step, step), step)
            part[j, rows, :] = part[j, rows, :] + read_code(got, slot, at(t, step), unit)
            return carry

        lax.fori_loop(0, tb // step, body, None)

    def ring(j, level, up, which):
        here = level if up else 3 - level
        out, got, s_sem, r_sem = (ups, upr, s_up, up_r) if up else (dns, dnr, s_dn, dn_r)
        toward = {"row": r + 1 if up else r - 1}
        far = [3, 2, 1, 0] if up else [0, 1, 2, 3]
        cond = r == here
        for n in which:
            b = far[n]
            i = j * 3 + (b - 1 if up else b)
            if b == here:

                @pl.when(cond)
                def _():
                    arrived(got.at[i], r_sem.at[i])
                    add_in(j, got, i)

                continue
            copy = pltpu.make_async_remote_copy(
                src_ref=out.at[i], dst_ref=got.at[i], send_sem=s_sem.at[i], recv_sem=r_sem.at[i],
                device_id=toward, device_id_type=MESH,
            )

            @pl.when(cond)
            def _():
                if level > 0:
                    arrived(got.at[i], r_sem.at[i])
                encode(j, b, out, i, got if level > 0 else None)
                copy.start()

            sent.append((copy.wait_send, cond))

    def level(j, n, which=None):
        which = range(4 - n if n else 3) if which is None else which
        ring(j, n, True, which)
        ring(j, n, False, which)

    def finish(j, cond):
        @pl.when(cond)
        def _():
            gi_out[j] = part[j, at(r, tb), :].astype(BF16)

        for i, q in enumerate(peers):
            send(
                gi_out.at[j, at(q, tl)], gi.at[:, at(c * CHUNKS + j, ic)],
                s_gi.at[j, i], gi_r.at[j, c], {"col": q}, cond,
            )
        local(gi_out.at[j, at(c, tl)], gi.at[:, at(c * CHUNKS + j, ic)], l_gi.at[j], cond)

    inner = jnp.logical_or(r == 1, r == 2)
    outer = jnp.logical_or(r == 0, r == 3)

    def run(name, f, *args):
        with jax.named_scope(name):
            f(*args)

    def mi(j):
        run("w_in%d" % j, weight_in, j)
        run("input%d" % j, multiply_input, j)

    def mw(j):
        run("pass%d_3" % j, pass_tokens, j, 3)
        run("weight%d" % j, multiply_weight, j)

    def lv(j, n, which=None):
        run("level%d_%d" % (j, n), level, j, n, which)

    def end(j, cond, name):
        run("end%d_%s" % (j, name), finish, j, cond)

    def block(n):
        run("from_core%d" % n, from_core, n)
        run("block%d" % n, multiply_block, 0, order[n])
        if n < 3:
            run("first%d" % n, level, 0, 0, [n])

    def ps(j, far):
        run("pass%d_%d" % (j, far), pass_tokens, j, far)

    run("mid0", pass_mid, 0)
    run("mid1", pass_mid, 1)
    for j in range(CHUNKS):
        run("own%d" % j, own_tokens_on, j)
    run("spread3", spread, 3)
    for n in range(3):
        run("spread%d" % n, spread, n)
    for j in range(1, CHUNKS):
        send_weight(j)
    run("crossed0", crossed, 0)
    ps(0, 1)
    run("crossed1", crossed, 1)
    run("to_core0", to_core, 0)
    ps(1, 1)
    run("crossed2", crossed, 2)
    run("crossed3", crossed, 3)
    run("w_in0", weight_in, 0)
    block(0)
    run("to_core1", to_core, 1)
    ps(2, 1)
    block(1)
    run("to_core2", to_core, 2)
    ps(3, 1)
    block(2)
    run("to_core3", to_core, 3)
    ps(0, 2)
    block(3)
    ps(1, 2)
    mi(1)
    lv(1, 0)
    ps(2, 2)
    lv(0, 1)
    mw(0)
    mi(2)
    lv(2, 0)
    ps(3, 2)
    lv(0, 2)
    end(0, inner, "in")
    lv(1, 1)
    mi(3)
    lv(3, 0)
    mw(1)
    lv(0, 3)
    end(0, outer, "out")
    lv(1, 2)
    end(1, inner, "in")
    mw(2)
    lv(2, 1)
    lv(1, 3)
    end(1, outer, "out")
    lv(2, 2)
    end(2, inner, "in")
    mw(3)
    lv(3, 1)
    lv(2, 3)
    end(2, outer, "out")
    lv(3, 2)
    end(3, inner, "in")
    lv(3, 3)
    end(3, outer, "out")

    def drain():
        for wait, cond in sent:
            when(cond, wait)

    def outputs():
        for j in range(CHUNKS):
            arrived(gi.at[:, at(c * CHUNKS + j, ic)], l_gi.at[j])
            arrived(gw.at[at(c * CHUNKS + j, ic)], l_gw.at[j])
            for q in peers:
                arrived(gi.at[:, at(q * CHUNKS + j, ic)], gi_r.at[j, q])
                arrived(gw.at[at(q * CHUNKS + j, ic)], gw_r.at[j, q])

    run("drain", drain)
    run("outputs", outputs)


def per_device_kernel(tokens, weight, grad_output):
    tl, il = tokens.shape
    ol = weight.shape[1]
    tb, ic = 4 * tl, il // (4 * CHUNKS)
    dma = pltpu.SemaphoreType.DMA
    code = pltpu.VMEM((3 * CHUNKS, tb + GROUP, ic), BF16)
    anywhere = pl.BlockSpec(memory_space=pl.ANY)
    return pl.pallas_call(
        kernel,
        out_shape=(
            jax.ShapeDtypeStruct(tokens.shape, BF16),
            jax.ShapeDtypeStruct(weight.shape, BF16),
        ),
        in_specs=[anywhere] * 3,
        out_specs=(anywhere, anywhere),
        scratch_shapes=[
            pltpu.VMEM((4 * tb, 4 * ol), BF16),
            pltpu.VMEM((2, tb // 2, ol), BF16),
            pltpu.VMEM((CHUNKS, 4 * tb, ic), BF16),
            pltpu.VMEM((ic, 4 * tb), BF16),
            pltpu.VMEM((CHUNKS, ic, 4 * ol), BF16),
            pltpu.VMEM((CHUNKS, 4 * tb, ic), F32),
            pltpu.VMEM((CHUNKS, ic, 4 * ol), BF16),
            pltpu.VMEM((CHUNKS, tb, ic), BF16),
            code, code, code, code,
            dma((2,)), dma((4,)), dma((4,)), dma((2, 4)), dma((4,)),
            dma((CHUNKS, 4)), dma((CHUNKS, 4)), dma((CHUNKS, 4)),
            dma((3 * CHUNKS,)), dma((3 * CHUNKS,)), dma((CHUNKS, 4)), dma((CHUNKS, 4)),
            dma((2,)), dma((4,)), dma((4,)), dma((2, 4)), dma((4,)),
            dma((CHUNKS, 3)), dma((CHUNKS, 3)), dma((CHUNKS, 2, 4)),
            dma((3 * CHUNKS,)), dma((3 * CHUNKS,)), dma((CHUNKS, 3)), dma((CHUNKS, 3)),
            dma((CHUNKS,)), dma((CHUNKS,)),
        ],
        compiler_params=pltpu.CompilerParams(
            collective_id=0, has_side_effects=True, vmem_limit_bytes=62 * 2**20
        ),
    )(tokens, weight, grad_output)


def solution(mesh):
    fours_fit = mesh.shape["row"] == 4 and mesh.shape["col"] == 4 and mesh.shape["depth"] == 2
    return jax.shard_map(
        per_device_kernel if fours_fit else per_device_general,
        mesh=mesh,
        in_specs=(
            P(("row", "col"), "depth"),
            P("depth", ("col", "row")),
            P("row", ("col", "depth")),
        ),
        out_specs=(P(("row", "col"), "depth"), P("depth", ("col", "row"))),
        check_vma=False,
    )
```

```python
import jax
import jax.numpy as jnp
from jax import lax
from jax.experimental import pallas as pl
from jax.experimental.pallas import tpu as pltpu
from jax.sharding import PartitionSpec as P

last_with_last = (((1,), (1,)), ((), ()))
first_with_first = (((0,), (0,)), ((), ()))
MESH = pl.DeviceIdType.MESH
CHUNKS = 4
GROUP = 16
SPAN = 83.0
TINY = 1e-30
F32, BF16 = jnp.float32, jnp.bfloat16


def input_grads(weight, grad_block):
    weight_block = lax.all_gather(weight, "row", axis=1, tiled=True)
    partial_value = lax.dot_general(
        grad_block, weight_block, last_with_last, preferred_element_type=jnp.float32
    )
    column_slab = lax.psum_scatter(partial_value, "col", scatter_dimension=1, tiled=True).astype(
        jnp.bfloat16
    )
    return lax.all_to_all(column_slab, "col", split_axis=0, concat_axis=1, tiled=True)


def weight_grads(tokens, grad_block):
    partial_value = lax.dot_general(
        lax.all_gather(tokens, "col", axis=0, tiled=True),
        grad_block,
        first_with_first,
        preferred_element_type=jnp.float32,
    )
    return lax.psum_scatter(partial_value, "row", scatter_dimension=1, tiled=True).astype(
        jnp.bfloat16
    )


def per_device_general(tokens, weight, grad_output):
    grad_block = lax.all_gather(grad_output, "depth", axis=1, tiled=True)
    grad_input = input_grads(weight, grad_block)
    grad_weight = weight_grads(tokens, grad_block)
    return (grad_input, grad_weight)


def place(c):
    return 2 * (c % 2) + c // 2


def kernel(
    tok, w, g, gi, gw,
    g_all, g_mid, x_all, x_t, w_all, part, gw_out, gi_out, ups, upr, dns, dnr,
    g_pre, g_z, g_x, g_y, g_d, x_r, w_r, x_z, up_r, dn_r, gi_r, gw_r,
    s_pre, s_z, s_x, s_y, s_d, s_xc, s_w, s_xz, s_up, s_dn, s_gi, s_gw, l_gi, l_gw,
):
    r, c, d = lax.axis_index("row"), lax.axis_index("col"), lax.axis_index("depth")
    k, x = c % 2, c // 2
    other = 1 - d
    core = c + 1 - 2 * k
    across = c + 2 - 4 * x
    diagonal = 3 - c
    peers = (across, diagonal, core)
    tl, il = tok.shape
    tb = 4 * tl
    half = tb // 2
    ib = il // 4
    ic = ib // CHUNKS
    ol = w.shape[1]

    barrier = pltpu.get_barrier_semaphore()
    for q in peers:
        pl.semaphore_signal(barrier, inc=1, device_id={"col": q}, device_id_type=MESH)
    pl.semaphore_signal(barrier, inc=1, device_id={"depth": other}, device_id_type=MESH)
    for s in (1, 2, 3):
        pl.semaphore_signal(barrier, inc=1, device_id={"row": (r + s) % 4}, device_id_type=MESH)
    pl.semaphore_wait(barrier, 7)

    sent = []

    def when(cond, f):
        if cond is None:
            f()
        else:
            pl.when(cond)(f)

    def send(src, dst, s_sem, r_sem, to, cond=None):
        copy = pltpu.make_async_remote_copy(
            src_ref=src, dst_ref=dst, send_sem=s_sem, recv_sem=r_sem, device_id=to, device_id_type=MESH
        )
        when(cond, copy.start)
        sent.append((copy.wait_send, cond))

    def local(src, dst, sem, cond=None):
        when(cond, pltpu.make_async_copy(src, dst, sem).start)

    def arrived(ref, sem, cond=None):
        when(cond, pltpu.make_async_copy(ref, ref, sem).wait)

    def at(i, n):
        return pl.ds(pl.multiple_of(i * n, n), n)

    def g_unit(s, h, q):
        return g_all.at[at(s * 2 + h, half), at(place(q), ol)]

    for h in (0, 1):
        to = 2 * d + h
        mine = to == r
        ours = g.at[at(d, half), at(h, ol)]
        theirs = g.at[at(other, half), at(h, ol)]
        send(theirs, g_unit(r, other, c), s_pre.at[h], g_z.at[r], {"depth": other}, mine)
        send(theirs, g_mid.at[h], s_pre.at[h], g_pre.at[h], {"depth": other}, jnp.logical_not(mine))
        local(ours, g_unit(r, d, c), g_z.at[r], mine)
        send(ours, g_unit(r, d, c), s_z.at[h], g_z.at[r], {"row": to}, jnp.logical_not(mine))

    def send_tokens(j):
        for i, q in enumerate(peers):
            send(
                tok.at[:, at(q * CHUNKS + j, ic)], x_all.at[j, at(r * 4 + c, tl)],
                s_xc.at[j, i], x_r.at[j, c], {"col": q},
            )
        local(tok.at[:, at(c * CHUNKS + j, ic)], x_all.at[j, at(r * 4 + c, tl)], x_r.at[j, c])

    def send_weight(j):
        for i, q in enumerate(peers):
            send(
                w.at[at(q * CHUNKS + j, ic)], w_all.at[j, :, at(place(c), ol)],
                s_w.at[j, i], w_r.at[j, c], {"col": q},
            )
        local(w.at[at(c * CHUNKS + j, ic)], w_all.at[j, :, at(place(c), ol)], w_r.at[j, c])

    for j in range(CHUNKS):
        send_tokens(j)
    send_weight(0)

    def tokens_on(j, s, direction, cond):
        block = x_all.at[j, at(s, tb)]
        send(block, block, s_xz.at[j, direction, s], x_z.at[j, s], {"row": r + 1 - 2 * direction}, cond)

    up_ok, down_ok = r < 3, r > 0

    def own_tokens_on(j):
        for q in range(4):
            arrived(x_all.at[j, at(r * 4 + q, tl)], x_r.at[j, q])
        tokens_on(j, r, 0, up_ok)
        tokens_on(j, r, 1, down_ok)

    def pass_tokens(j, far):
        below, above = r - far, r + far
        low, high = jnp.maximum(below, 0), jnp.minimum(above, 3)
        has_low, has_high = below >= 0, above <= 3
        arrived(x_all.at[j, at(low, tb)], x_z.at[j, low], has_low)
        tokens_on(j, low, 0, jnp.logical_and(has_low, up_ok))
        arrived(x_all.at[j, at(high, tb)], x_z.at[j, high], has_high)
        tokens_on(j, high, 1, jnp.logical_and(has_high, down_ok))

    near = 3 * (1 - r // 2)
    last = 1 + r % 2
    order = [near, 6 - r - near - last, last, r]

    def spread(n):
        s = order[n]
        unit = g_unit(s, d, c)
        arrived(unit, g_z.at[s])
        send(unit, unit, s_x.at[s], g_x.at[s], {"col": across})
        send(unit, unit, s_y.at[0, s], g_y.at[0, s], {"depth": other})

    def crossed(n):
        s = order[n]
        unit = g_unit(s, d, across)
        arrived(unit, g_x.at[s])
        send(unit, unit, s_y.at[1, s], g_y.at[1, s], {"depth": other})

    def to_core(n):
        s = order[n]
        arrived(g_unit(s, other, c), g_y.at[0, s])
        arrived(g_unit(s, other, across), g_y.at[1, s])
        slab = g_all.at[at(s, tb), at(k, 2 * ol)]
        send(slab, slab, s_d.at[s], g_d.at[s], {"col": core})

    def pass_mid(h):
        to = 2 * other + h
        go = to != r
        arrived(g_mid.at[h], g_pre.at[h], go)
        send(g_mid.at[h], g_unit(r, d, c), s_z.at[2 + h], g_z.at[r], {"row": to}, go)

    def from_core(n):
        s = order[n]
        arrived(g_all.at[at(s, tb), at(1 - k, 2 * ol)], g_d.at[s])

    def weight_in(j):
        for q in range(4):
            arrived(w_all.at[j, :, at(place(q), ol)], w_r.at[j, q])

    def multiply_block(j, s):
        rows = at(s, tb)
        part[j, rows, :] = lax.dot_general(
            g_all[rows, :], w_all[j], last_with_last, preferred_element_type=F32
        )

    def multiply_input(j):
        def body(b, carry):
            multiply_block(j, b)
            return carry

        lax.fori_loop(0, 4, body, None)

    def multiply_weight(j):
        def turn(b, carry):
            x_t[:, at(b, half)] = x_all[j, at(b, half), :].T
            return carry

        lax.fori_loop(0, 8, turn, None)

        def body(n, carry):
            cols = at(n, ol)
            gw_out[j, :, cols] = jnp.dot(
                x_t[...], g_all[:, cols], preferred_element_type=F32
            ).astype(BF16)
            return carry

        lax.fori_loop(0, 4, body, None)
        for i, q in enumerate(peers):
            send(
                gw_out.at[j, :, at(place(q), ol)], gw.at[at(c * CHUNKS + j, ic)],
                s_gw.at[j, i], gw_r.at[j, c], {"col": q},
            )
        local(gw_out.at[j, :, at(place(c), ol)], gw.at[at(c * CHUNKS + j, ic)], l_gw.at[j])

    step = 64
    scale_rows = pl.ds(tb, GROUP)

    def read_code(buf, i, rows, unit):
        v = buf[i, rows, :].astype(F32)
        size = jnp.log(jnp.abs(v)) + SPAN
        size = size * jnp.concatenate([unit] * (step // GROUP), axis=0)
        return jnp.where(v < 0, -size, size)

    def unit_of(buf, i):
        return buf[i, scale_rows, :].astype(F32) * (0.5 / SPAN)

    def encode(j, b, out, slot, got):
        unit = None if got is None else unit_of(got, slot)

        def total(t):
            value = part[j, pl.ds(pl.multiple_of(b * tb + t * step, step), step), :]
            if got is not None:
                value = value + read_code(got, slot, at(t, step), unit)
            return value

        def first(t, most):
            value = total(t)
            if got is not None:
                part[j, pl.ds(pl.multiple_of(b * tb + t * step, step), step), :] = value
            size = jnp.abs(value)
            for n in range(step // GROUP):
                most = jnp.maximum(most, size[n * GROUP : (n + 1) * GROUP])
            return most

        most = lax.fori_loop(0, tb // step, first, jnp.full((GROUP, ic), TINY, F32))
        scale = (most * 1.01).astype(BF16)
        out[slot, scale_rows, :] = scale
        by = (2 * SPAN) / scale.astype(F32)
        by = jnp.concatenate([by] * (step // GROUP), axis=0)

        def second(t, carry):
            value = part[j, pl.ds(pl.multiple_of(b * tb + t * step, step), step), :]
            code = jnp.exp(jnp.abs(value) * by - SPAN)
            out[slot, at(t, step), :] = jnp.where(value < 0, -code, code).astype(BF16)
            return carry

        lax.fori_loop(0, tb // step, second, None)

    def add_in(j, got, slot):
        unit = unit_of(got, slot)

        def body(t, carry):
            rows = pl.ds(pl.multiple_of(r * tb + t * step, step), step)
            part[j, rows, :] = part[j, rows, :] + read_code(got, slot, at(t, step), unit)
            return carry

        lax.fori_loop(0, tb // step, body, None)

    def ring(j, level, up, which):
        here = level if up else 3 - level
        out, got, s_sem, r_sem = (ups, upr, s_up, up_r) if up else (dns, dnr, s_dn, dn_r)
        toward = {"row": r + 1 if up else r - 1}
        far = [3, 2, 1, 0] if up else [0, 1, 2, 3]
        cond = r == here
        for n in which:
            b = far[n]
            i = j * 3 + (b - 1 if up else b)
            if b == here:

                @pl.when(cond)
                def _():
                    arrived(got.at[i], r_sem.at[i])
                    add_in(j, got, i)

                continue
            copy = pltpu.make_async_remote_copy(
                src_ref=out.at[i], dst_ref=got.at[i], send_sem=s_sem.at[i], recv_sem=r_sem.at[i],
                device_id=toward, device_id_type=MESH,
            )

            @pl.when(cond)
            def _():
                if level > 0:
                    arrived(got.at[i], r_sem.at[i])
                encode(j, b, out, i, got if level > 0 else None)
                copy.start()

            sent.append((copy.wait_send, cond))

    def level(j, n, which=None):
        which = range(4 - n if n else 3) if which is None else which
        ring(j, n, True, which)
        ring(j, n, False, which)

    def finish(j, cond):
        @pl.when(cond)
        def _():
            gi_out[j] = part[j, at(r, tb), :].astype(BF16)

        for i, q in enumerate(peers):
            send(
                gi_out.at[j, at(q, tl)], gi.at[:, at(c * CHUNKS + j, ic)],
                s_gi.at[j, i], gi_r.at[j, c], {"col": q}, cond,
            )
        local(gi_out.at[j, at(c, tl)], gi.at[:, at(c * CHUNKS + j, ic)], l_gi.at[j], cond)

    inner = jnp.logical_or(r == 1, r == 2)
    outer = jnp.logical_or(r == 0, r == 3)

    def run(name, f, *args):
        with jax.named_scope(name):
            f(*args)

    def mi(j):
        run("w_in%d" % j, weight_in, j)
        run("input%d" % j, multiply_input, j)

    def mw(j):
        run("pass%d_3" % j, pass_tokens, j, 3)
        run("weight%d" % j, multiply_weight, j)

    def lv(j, n, which=None):
        run("level%d_%d" % (j, n), level, j, n, which)

    def end(j, cond, name):
        run("end%d_%s" % (j, name), finish, j, cond)

    def block(n):
        run("from_core%d" % n, from_core, n)
        run("block%d" % n, multiply_block, 0, order[n])
        if n < 3:
            run("first%d" % n, level, 0, 0, [n])

    def ps(j, far):
        run("pass%d_%d" % (j, far), pass_tokens, j, far)

    run("mid0", pass_mid, 0)
    run("mid1", pass_mid, 1)
    for j in range(CHUNKS):
        run("own%d" % j, own_tokens_on, j)
    run("spread3", spread, 3)
    for n in range(3):
        run("spread%d" % n, spread, n)
    for j in range(1, CHUNKS):
        send_weight(j)
    run("crossed0", crossed, 0)
    ps(0, 1)
    run("crossed1", crossed, 1)
    run("to_core0", to_core, 0)
    ps(1, 1)
    run("crossed2", crossed, 2)
    run("crossed3", crossed, 3)
    run("w_in0", weight_in, 0)
    block(0)
    run("to_core1", to_core, 1)
    ps(2, 1)
    block(1)
    run("to_core2", to_core, 2)
    ps(3, 1)
    block(2)
    run("to_core3", to_core, 3)
    ps(0, 2)
    block(3)
    ps(1, 2)
    mi(1)
    lv(1, 0)
    ps(2, 2)
    lv(0, 1)
    mw(0)
    mi(2)
    lv(2, 0)
    ps(3, 2)
    lv(0, 2)
    end(0, inner, "in")
    lv(1, 1)
    mi(3)
    lv(3, 0)
    mw(1)
    lv(0, 3)
    end(0, outer, "out")
    lv(1, 2)
    end(1, inner, "in")
    mw(2)
    lv(2, 1)
    lv(1, 3)
    end(1, outer, "out")
    lv(2, 2)
    end(2, inner, "in")
    mw(3)
    lv(3, 1)
    lv(2, 3)
    end(2, outer, "out")
    lv(3, 2)
    end(3, inner, "in")
    lv(3, 3)
    end(3, outer, "out")

    def drain():
        for wait, cond in sent:
            when(cond, wait)

    def outputs():
        for j in range(CHUNKS):
            arrived(gi.at[:, at(c * CHUNKS + j, ic)], l_gi.at[j])
            arrived(gw.at[at(c * CHUNKS + j, ic)], l_gw.at[j])
            for q in peers:
                arrived(gi.at[:, at(q * CHUNKS + j, ic)], gi_r.at[j, q])
                arrived(gw.at[at(q * CHUNKS + j, ic)], gw_r.at[j, q])

    run("drain", drain)
    run("outputs", outputs)


def per_device_kernel(tokens, weight, grad_output):
    tl, il = tokens.shape
    ol = weight.shape[1]
    tb, ic = 4 * tl, il // (4 * CHUNKS)
    dma = pltpu.SemaphoreType.DMA
    code = pltpu.VMEM((3 * CHUNKS, tb + GROUP, ic), BF16)
    anywhere = pl.BlockSpec(memory_space=pl.ANY)
    return pl.pallas_call(
        kernel,
        out_shape=(
            jax.ShapeDtypeStruct(tokens.shape, BF16),
            jax.ShapeDtypeStruct(weight.shape, BF16),
        ),
        in_specs=[anywhere] * 3,
        out_specs=(anywhere, anywhere),
        scratch_shapes=[
            pltpu.VMEM((4 * tb, 4 * ol), BF16),
            pltpu.VMEM((2, tb // 2, ol), BF16),
            pltpu.VMEM((CHUNKS, 4 * tb, ic), BF16),
            pltpu.VMEM((ic, 4 * tb), BF16),
            pltpu.VMEM((CHUNKS, ic, 4 * ol), BF16),
            pltpu.VMEM((CHUNKS, 4 * tb, ic), F32),
            pltpu.VMEM((CHUNKS, ic, 4 * ol), BF16),
            pltpu.VMEM((CHUNKS, tb, ic), BF16),
            code, code, code, code,
            dma((2,)), dma((4,)), dma((4,)), dma((2, 4)), dma((4,)),
            dma((CHUNKS, 4)), dma((CHUNKS, 4)), dma((CHUNKS, 4)),
            dma((3 * CHUNKS,)), dma((3 * CHUNKS,)), dma((CHUNKS, 4)), dma((CHUNKS, 4)),
            dma((2,)), dma((4,)), dma((4,)), dma((2, 4)), dma((4,)),
            dma((CHUNKS, 3)), dma((CHUNKS, 3)), dma((CHUNKS, 2, 4)),
            dma((3 * CHUNKS,)), dma((3 * CHUNKS,)), dma((CHUNKS, 3)), dma((CHUNKS, 3)),
            dma((CHUNKS,)), dma((CHUNKS,)),
        ],
        compiler_params=pltpu.CompilerParams(
            collective_id=0, has_side_effects=True, vmem_limit_bytes=46 * 2**20
        ),
    )(*[pltpu.with_memory_space_constraint(a, pltpu.HBM) for a in (tokens, weight, grad_output)])


def solution(mesh):
    fours_fit = mesh.shape["row"] == 4 and mesh.shape["col"] == 4 and mesh.shape["depth"] == 2
    return jax.shard_map(
        per_device_kernel if fours_fit else per_device_general,
        mesh=mesh,
        in_specs=(
            P(("row", "col"), "depth"),
            P("depth", ("col", "row")),
            P("row", ("col", "depth")),
        ),
        out_specs=(P(("row", "col"), "depth"), P("depth", ("col", "row"))),
        check_vma=False,
    )
```

```python
import jax
import jax.numpy as jnp
from jax import lax
from jax.experimental import pallas as pl
from jax.experimental.pallas import tpu as pltpu
from jax.sharding import PartitionSpec as P

last_with_last = (((1,), (1,)), ((), ()))
first_with_first = (((0,), (0,)), ((), ()))
MESH = pl.DeviceIdType.MESH
CHUNKS = 4
GROUP = 16
SPAN = 83.0
TINY = 1e-30
F32, BF16 = jnp.float32, jnp.bfloat16


def input_grads(weight, grad_block):
    weight_block = lax.all_gather(weight, "row", axis=1, tiled=True)
    partial_value = lax.dot_general(
        grad_block, weight_block, last_with_last, preferred_element_type=jnp.float32
    )
    column_slab = lax.psum_scatter(partial_value, "col", scatter_dimension=1, tiled=True).astype(
        jnp.bfloat16
    )
    return lax.all_to_all(column_slab, "col", split_axis=0, concat_axis=1, tiled=True)


def weight_grads(tokens, grad_block):
    partial_value = lax.dot_general(
        lax.all_gather(tokens, "col", axis=0, tiled=True),
        grad_block,
        first_with_first,
        preferred_element_type=jnp.float32,
    )
    return lax.psum_scatter(partial_value, "row", scatter_dimension=1, tiled=True).astype(
        jnp.bfloat16
    )


def per_device_general(tokens, weight, grad_output):
    grad_block = lax.all_gather(grad_output, "depth", axis=1, tiled=True)
    grad_input = input_grads(weight, grad_block)
    grad_weight = weight_grads(tokens, grad_block)
    return (grad_input, grad_weight)


def place(c):
    return 2 * (c % 2) + c // 2


def kernel(
    tok, w, g, gi, gw,
    g_all, g_mid, x_all, x_t, w_all, part, gw_out, gi_out, ups, upr, dns, dnr,
    g_pre, g_z, g_x, g_y, g_d, x_r, w_r, x_z, up_r, dn_r, gi_r, gw_r,
    s_pre, s_z, s_x, s_y, s_d, s_xc, s_w, s_xz, s_up, s_dn, s_gi, s_gw, l_gi, l_gw, come,
):
    r, c, d = lax.axis_index("row"), lax.axis_index("col"), lax.axis_index("depth")
    k, x = c % 2, c // 2
    other = 1 - d
    core = c + 1 - 2 * k
    across = c + 2 - 4 * x
    diagonal = 3 - c
    peers = (across, diagonal, core)
    tl, il = tok.shape
    tb = 4 * tl
    half = tb // 2
    ib = il // 4
    ic = ib // CHUNKS
    ol = w.shape[1]

    up_ok, down_ok = r < 3, r > 0
    inner, outer = jnp.logical_and(up_ok, down_ok), jnp.logical_or(r == 0, r == 3)

    def tell(sem, to, cond=None):
        when(cond, lambda: pl.semaphore_signal(sem, inc=1, device_id=to, device_id_type=MESH))

    def when(cond, f):
        if cond is None:
            f()
        else:
            pl.when(cond)(f)

    barrier = pltpu.get_barrier_semaphore()
    for q in peers:
        tell(barrier, {"col": q})
    tell(barrier, {"depth": other})
    tell(barrier, {"row": r + 1}, up_ok)
    tell(barrier, {"row": r - 1}, down_ok)
    when(inner, lambda: pl.semaphore_wait(barrier, 6))
    when(outer, lambda: pl.semaphore_wait(barrier, 5))
    tell(come.at[0], {"row": r + 1}, inner)
    tell(come.at[1], {"row": r - 1}, inner)

    def all_in():
        @pl.when(r >= 2)
        def _():
            pl.semaphore_wait(come.at[0], 1)

        @pl.when(r <= 1)
        def _():
            pl.semaphore_wait(come.at[1], 1)

        tell(come.at[2], {"row": r + 1}, r == 2)
        tell(come.at[2], {"row": r - 1}, r == 1)

        @pl.when(outer)
        def _():
            pl.semaphore_wait(come.at[2], 1)

    sent = []

    def send(src, dst, s_sem, r_sem, to, cond=None):
        copy = pltpu.make_async_remote_copy(
            src_ref=src, dst_ref=dst, send_sem=s_sem, recv_sem=r_sem, device_id=to, device_id_type=MESH
        )
        when(cond, copy.start)
        sent.append((copy.wait_send, cond))

    def local(src, dst, sem, cond=None):
        when(cond, pltpu.make_async_copy(src, dst, sem).start)

    def arrived(ref, sem, cond=None):
        when(cond, pltpu.make_async_copy(ref, ref, sem).wait)

    def at(i, n):
        return pl.ds(pl.multiple_of(i * n, n), n)

    def g_unit(s, h, q):
        return g_all.at[at(s * 2 + h, half), at(place(q), ol)]

    def far_first(depth):
        return depth, 1 - depth

    for h in far_first(d):
        to = 2 * d + h
        mine = to == r
        ours = g.at[at(d, half), at(h, ol)]
        theirs = g.at[at(other, half), at(h, ol)]
        send(theirs, g_unit(r, other, c), s_pre.at[h], g_z.at[r], {"depth": other}, mine)
        send(theirs, g_mid.at[h], s_pre.at[h], g_pre.at[h], {"depth": other}, jnp.logical_not(mine))
        local(ours, g_unit(r, d, c), g_z.at[r], mine)
        near = jnp.logical_or(to == r + 1, to == r - 1)
        send(ours, g_unit(r, d, c), s_z.at[h], g_z.at[r], {"row": to}, near)

    def features(q, j):
        return at(q * CHUNKS + j, ic)

    def send_tokens(j):
        for i, q in enumerate(peers):
            send(
                tok.at[:, features(q, j)], x_all.at[j, at(r * 4 + c, tl)],
                s_xc.at[j, i], x_r.at[j, c], {"col": q},
            )
        local(tok.at[:, features(c, j)], x_all.at[j, at(r * 4 + c, tl)], x_r.at[j, c])

    def send_weight(j):
        for i, q in enumerate(peers):
            send(
                w.at[at(q * CHUNKS + j, ic)], w_all.at[j, :, at(place(c), ol)],
                s_w.at[j, i], w_r.at[j, c], {"col": q},
            )
        local(w.at[at(c * CHUNKS + j, ic)], w_all.at[j, :, at(place(c), ol)], w_r.at[j, c])

    for j in range(CHUNKS):
        send_tokens(j)
    send_weight(0)

    all_in()
    for h in far_first(d):
        to = 2 * d + h
        away = jnp.logical_or(to > r + 1, to < r - 1)
        send(g.at[at(d, half), at(h, ol)], g_unit(r, d, c), s_z.at[h], g_z.at[r], {"row": to}, away)

    def tokens_on(j, s, direction, cond):
        block = x_all.at[j, at(s, tb)]
        send(block, block, s_xz.at[j, direction, s], x_z.at[j, s], {"row": r + 1 - 2 * direction}, cond)

    def own_tokens_on(j):
        for q in range(4):
            arrived(x_all.at[j, at(r * 4 + q, tl)], x_r.at[j, q])
        tokens_on(j, r, 0, up_ok)
        tokens_on(j, r, 1, down_ok)

    def pass_tokens(j, far):
        below, above = r - far, r + far
        low, high = jnp.maximum(below, 0), jnp.minimum(above, 3)
        has_low, has_high = below >= 0, above <= 3
        arrived(x_all.at[j, at(low, tb)], x_z.at[j, low], has_low)
        tokens_on(j, low, 0, jnp.logical_and(has_low, up_ok))
        arrived(x_all.at[j, at(high, tb)], x_z.at[j, high], has_high)
        tokens_on(j, high, 1, jnp.logical_and(has_high, down_ok))

    near = 3 * (1 - r // 2)
    last = 1 + r % 2
    order = [near, 6 - r - near - last, last, r]

    def spread(n):
        s = order[n]
        unit = g_unit(s, d, c)
        arrived(unit, g_z.at[s])
        send(unit, unit, s_y.at[0, s], g_y.at[0, s], {"depth": other})
        if n < 3:
            spread_across(n)

    def spread_across(n):
        s = order[n]
        unit = g_unit(s, d, c)
        send(unit, unit, s_x.at[s], g_x.at[s], {"col": across})

    def crossed(n):
        s = order[n]
        unit = g_unit(s, d, across)
        arrived(unit, g_x.at[s])
        send(unit, unit, s_y.at[1, s], g_y.at[1, s], {"depth": other})

    def to_core(n):
        s = order[n]
        arrived(g_unit(s, other, c), g_y.at[0, s])
        arrived(g_unit(s, other, across), g_y.at[1, s])
        slab = g_all.at[at(s, tb), at(k, 2 * ol)]
        send(slab, slab, s_d.at[s], g_d.at[s], {"col": core})

    def pass_mid(i):
        h = far_first(other)[i]
        to = 2 * other + h
        go = to != r
        arrived(g_mid.at[h], g_pre.at[h], go)
        send(g_mid.at[h], g_unit(r, d, c), s_z.at[2 + h], g_z.at[r], {"row": to}, go)

    def from_core(n):
        s = order[n]
        arrived(g_all.at[at(s, tb), at(1 - k, 2 * ol)], g_d.at[s])

    def weight_in(j):
        for q in range(4):
            arrived(w_all.at[j, :, at(place(q), ol)], w_r.at[j, q])

    def multiply_block(j, s):
        rows = at(s, tb)
        part[j, rows, :] = lax.dot_general(
            g_all[rows, :], w_all[j], last_with_last, preferred_element_type=F32
        )

    def multiply_input(j):
        def body(b, carry):
            multiply_block(j, b)
            return carry

        lax.fori_loop(0, 4, body, None)

    def turn_tokens(j):
        def turn(b, carry):
            x_t[:, at(b, half)] = x_all[j, at(b, half), :].T
            return carry

        lax.fori_loop(0, 8, turn, None)

    def multiply_columns(j, q_from, q_to):
        gw_out[j, :, at(q_to, ol)] = jnp.dot(
            x_t[...], g_all[:, at(q_from, ol)], preferred_element_type=F32
        ).astype(BF16)

    def multiply_weight(j):
        turn_tokens(j)

        def body(n, carry):
            multiply_columns(j, n, n)
            return carry

        lax.fori_loop(0, 4, body, None)
        for i, q in enumerate(peers):
            send(
                gw_out.at[j, :, at(place(q), ol)], gw.at[features(c, j)],
                s_gw.at[j, i], gw_r.at[j, c], {"col": q},
            )
        local(gw_out.at[j, :, at(place(c), ol)], gw.at[features(c, j)], l_gw.at[j])

    step = 64
    scale_rows = pl.ds(tb, GROUP)

    def read_code(buf, i, rows, unit):
        v = buf[i, rows, :].astype(F32)
        size = jnp.log(jnp.abs(v)) + SPAN
        size = size * jnp.concatenate([unit] * (step // GROUP), axis=0)
        return jnp.where(v < 0, -size, size)

    def unit_of(buf, i):
        return buf[i, scale_rows, :].astype(F32) * (0.5 / SPAN)

    def encode(j, b, out, slot, got):
        unit = None if got is None else unit_of(got, slot)

        def total(t):
            value = part[j, pl.ds(pl.multiple_of(b * tb + t * step, step), step), :]
            if got is not None:
                value = value + read_code(got, slot, at(t, step), unit)
            return value

        def first(t, most):
            value = total(t)
            if got is not None:
                part[j, pl.ds(pl.multiple_of(b * tb + t * step, step), step), :] = value
            size = jnp.abs(value)
            for n in range(step // GROUP):
                most = jnp.maximum(most, size[n * GROUP : (n + 1) * GROUP])
            return most

        most = lax.fori_loop(0, tb // step, first, jnp.full((GROUP, ic), TINY, F32))
        scale = (most * 1.01).astype(BF16)
        out[slot, scale_rows, :] = scale
        by = (2 * SPAN) / scale.astype(F32)
        by = jnp.concatenate([by] * (step // GROUP), axis=0)

        def second(t, carry):
            value = part[j, pl.ds(pl.multiple_of(b * tb + t * step, step), step), :]
            code = jnp.exp(jnp.abs(value) * by - SPAN)
            out[slot, at(t, step), :] = jnp.where(value < 0, -code, code).astype(BF16)
            return carry

        lax.fori_loop(0, tb // step, second, None)

    def add_in(j, got, slot):
        unit = unit_of(got, slot)

        def body(t, carry):
            rows = pl.ds(pl.multiple_of(r * tb + t * step, step), step)
            part[j, rows, :] = part[j, rows, :] + read_code(got, slot, at(t, step), unit)
            return carry

        lax.fori_loop(0, tb // step, body, None)

    def ring(j, level, up, which):
        here = level if up else 3 - level
        out, got, s_sem, r_sem = (ups, upr, s_up, up_r) if up else (dns, dnr, s_dn, dn_r)
        toward = {"row": r + 1 if up else r - 1}
        far = [3, 2, 1, 0] if up else [0, 1, 2, 3]
        cond = r == here
        for n in which:
            b = far[n]
            i = j * 3 + (b - 1 if up else b)
            if b == here:

                @pl.when(cond)
                def _():
                    arrived(got.at[i], r_sem.at[i])
                    add_in(j, got, i)

                continue
            copy = pltpu.make_async_remote_copy(
                src_ref=out.at[i], dst_ref=got.at[i], send_sem=s_sem.at[i], recv_sem=r_sem.at[i],
                device_id=toward, device_id_type=MESH,
            )

            @pl.when(cond)
            def _():
                if level > 0:
                    arrived(got.at[i], r_sem.at[i])
                encode(j, b, out, i, got if level > 0 else None)
                copy.start()

            sent.append((copy.wait_send, cond))

    def level(j, n, which=None):
        which = range(4 - n if n else 3) if which is None else which
        ring(j, n, True, which)
        ring(j, n, False, which)

    def finish(j, cond):
        @pl.when(cond)
        def _():
            gi_out[j] = part[j, at(r, tb), :].astype(BF16)

        for i, q in enumerate(peers):
            send(
                gi_out.at[j, at(q, tl)], gi.at[:, at(c * CHUNKS + j, ic)],
                s_gi.at[j, i], gi_r.at[j, c], {"col": q}, cond,
            )
        local(gi_out.at[j, at(c, tl)], gi.at[:, at(c * CHUNKS + j, ic)], l_gi.at[j], cond)

    def run(name, f, *args):
        with jax.named_scope(name):
            f(*args)

    def mi(j):
        run("w_in%d" % j, weight_in, j)
        run("input%d" % j, multiply_input, j)

    def mw(j):
        run("pass%d_3" % j, pass_tokens, j, 3)
        run("weight%d" % j, multiply_weight, j)

    def lv(j, n, which=None):
        run("level%d_%d" % (j, n), level, j, n, which)

    def end(j, cond, name):
        run("end%d_%s" % (j, name), finish, j, cond)

    def block(n):
        run("from_core%d" % n, from_core, n)
        run("block%d" % n, multiply_block, 0, order[n])
        if n < 3:
            run("first%d" % n, level, 0, 0, [n])

    def ps(j, far):
        run("pass%d_%d" % (j, far), pass_tokens, j, far)

    def l0(j, n):
        run("l0_%d%d" % (j, n), level, j, 0, [n])

    def l1(j, n):
        run("l1_%d%d" % (j, n), level, j, 1, [n])

    def l2(j, n):
        run("l2_%d%d" % (j, n), level, j, 2, [n])

    def l3(j):
        run("l3_%d" % j, level, j, 3, [0])
        end(j, outer, "out")

    def some(j, n):
        run("blk%d_%d" % (j, n), multiply_block, j, order[n])

    run("mid0", pass_mid, 0)
    run("spread3", spread, 3)
    run("mid1", pass_mid, 1)
    run("own0", own_tokens_on, 0)
    run("own1", own_tokens_on, 1)
    for n in range(3):
        run("spread%d" % n, spread, n)
    spread_across(3)
    for j in range(1, CHUNKS):
        send_weight(j)
    run("own2", own_tokens_on, 2)
    ps(0, 1)
    run("own3", own_tokens_on, 3)
    run("crossed0", crossed, 0)
    run("crossed1", crossed, 1)
    ps(1, 1)
    run("crossed2", crossed, 2)
    ps(2, 1)
    run("to_core0", to_core, 0)
    run("w_in0", weight_in, 0)
    block(0)
    run("to_core1", to_core, 1)
    run("crossed3", crossed, 3)
    ps(0, 2)
    block(1)
    ps(3, 1)
    run("to_core2", to_core, 2)
    block(2)
    l1(0, 0)
    run("to_core3", to_core, 3)
    ps(1, 2)
    run("w_in1", weight_in, 1)
    for n in range(3):
        some(1, n)
        l0(1, n)
    block(3)
    some(1, 3)
    l1(0, 1)
    l1(0, 2)
    ps(2, 2)
    mw(0)
    mi(2)
    for n in range(3):
        l0(2, n)
    l1(1, 0)
    l2(0, 0)
    l1(1, 1)
    l2(0, 1)
    end(0, inner, "in")
    l1(1, 2)
    ps(3, 2)
    mw(1)
    mi(3)
    for n in range(3):
        l0(3, n)
    l3(0)
    l2(1, 0)
    l1(2, 0)
    l2(1, 1)
    end(1, inner, "in")
    mw(2)
    l1(2, 1)
    l3(1)
    l1(2, 2)
    l2(2, 0)
    l2(2, 1)
    end(2, inner, "in")
    mw(3)
    l1(3, 0)
    l3(2)
    l1(3, 1)
    l1(3, 2)
    l2(3, 0)
    l2(3, 1)
    end(3, inner, "in")
    l3(3)

    def drain():
        for wait, cond in sent:
            when(cond, wait)

    def outputs():
        for j in range(CHUNKS):
            arrived(gi.at[:, features(c, j)], l_gi.at[j])
            arrived(gw.at[features(c, j)], l_gw.at[j])
            for q in peers:
                arrived(gi.at[:, features(q, j)], gi_r.at[j, q])
                arrived(gw.at[features(q, j)], gw_r.at[j, q])

    run("drain", drain)
    run("outputs", outputs)


def per_device_kernel(tokens, weight, grad_output):
    tl, il = tokens.shape
    ol = weight.shape[1]
    tb, ic = 4 * tl, il // (4 * CHUNKS)
    dma = pltpu.SemaphoreType.DMA
    code = pltpu.VMEM((3 * CHUNKS, tb + GROUP, ic), BF16)
    anywhere = pl.BlockSpec(memory_space=pl.ANY)
    return pl.pallas_call(
        kernel,
        out_shape=(
            jax.ShapeDtypeStruct(tokens.shape, BF16),
            jax.ShapeDtypeStruct(weight.shape, BF16),
        ),
        in_specs=[anywhere] * 3,
        out_specs=(anywhere, anywhere),
        scratch_shapes=[
            pltpu.VMEM((4 * tb, 4 * ol), BF16),
            pltpu.VMEM((2, tb // 2, ol), BF16),
            pltpu.VMEM((CHUNKS, 4 * tb, ic), BF16),
            pltpu.VMEM((ic, 4 * tb), BF16),
            pltpu.VMEM((CHUNKS, ic, 4 * ol), BF16),
            pltpu.VMEM((CHUNKS, 4 * tb, ic), F32),
            pltpu.VMEM((CHUNKS, ic, 4 * ol), BF16),
            pltpu.VMEM((CHUNKS, tb, ic), BF16),
            code, code, code, code,
            dma((2,)), dma((4,)), dma((4,)), dma((2, 4)), dma((4,)),
            dma((CHUNKS, 4)), dma((CHUNKS, 4)), dma((CHUNKS, 4)),
            dma((3 * CHUNKS,)), dma((3 * CHUNKS,)), dma((CHUNKS, 4)), dma((CHUNKS, 4)),
            dma((2,)), dma((4,)), dma((4,)), dma((2, 4)), dma((4,)),
            dma((CHUNKS, 3)), dma((CHUNKS, 3)), dma((CHUNKS, 2, 4)),
            dma((3 * CHUNKS,)), dma((3 * CHUNKS,)), dma((CHUNKS, 3)), dma((CHUNKS, 3)),
            dma((CHUNKS,)), dma((CHUNKS,)), pltpu.SemaphoreType.REGULAR((3,)),
        ],
        compiler_params=pltpu.CompilerParams(
            collective_id=0, has_side_effects=True, vmem_limit_bytes=46 * 2**20
        ),
    )(*[pltpu.with_memory_space_constraint(a, pltpu.HBM) for a in (tokens, weight, grad_output)])


def solution(mesh):
    fours_fit = mesh.shape["row"] == 4 and mesh.shape["col"] == 4 and mesh.shape["depth"] == 2
    return jax.shard_map(
        per_device_kernel if fours_fit else per_device_general,
        mesh=mesh,
        in_specs=(
            P(("row", "col"), "depth"),
            P("depth", ("col", "row")),
            P("row", ("col", "depth")),
        ),
        out_specs=(P(("row", "col"), "depth"), P("depth", ("col", "row"))),
        check_vma=False,
    )
```

```python
import jax
import jax.numpy as jnp
from jax import lax
from jax.experimental import pallas as pl
from jax.experimental.pallas import tpu as pltpu
from jax.sharding import PartitionSpec as P

last_with_last = (((1,), (1,)), ((), ()))
first_with_first = (((0,), (0,)), ((), ()))
MESH = pl.DeviceIdType.MESH
PRE, Z, X, Y, CORE, TOK, HOME, W, UP, DOWN, TOK_UP, TOK_DOWN, HOME_UP, HOME_DOWN, GI, GW = range(16)
CHUNKS = 4
LAST = CHUNKS - 1
GROUP = 16
SPAN = 83.0
TINY = 1e-30
F32, BF16 = jnp.float32, jnp.bfloat16


def input_grads(weight, grad_block):
    weight_block = lax.all_gather(weight, "row", axis=1, tiled=True)
    partial_value = lax.dot_general(
        grad_block, weight_block, last_with_last, preferred_element_type=jnp.float32
    )
    column_slab = lax.psum_scatter(partial_value, "col", scatter_dimension=1, tiled=True).astype(
        jnp.bfloat16
    )
    return lax.all_to_all(column_slab, "col", split_axis=0, concat_axis=1, tiled=True)


def weight_grads(tokens, grad_block):
    partial_value = lax.dot_general(
        lax.all_gather(tokens, "col", axis=0, tiled=True),
        grad_block,
        first_with_first,
        preferred_element_type=jnp.float32,
    )
    return lax.psum_scatter(partial_value, "row", scatter_dimension=1, tiled=True).astype(
        jnp.bfloat16
    )


def per_device_general(tokens, weight, grad_output):
    grad_block = lax.all_gather(grad_output, "depth", axis=1, tiled=True)
    grad_input = input_grads(weight, grad_block)
    grad_weight = weight_grads(tokens, grad_block)
    return (grad_input, grad_weight)


def place(c):
    return 2 * (c % 2) + c // 2


def kernel(
    tok, w, g, gi, gw,
    g_all, g_mid, x_all, x_t, w_all, part, gw_out, gi_out, ups, upr, dns, dnr,
    x_home, come, g_pre, g_z, g_x, g_y, g_d, x_r, w_r, x_z, up_r, dn_r, done, gone,
):
    r, c, d = lax.axis_index("row"), lax.axis_index("col"), lax.axis_index("depth")
    k, x = c % 2, c // 2
    other = 1 - d
    core = c + 1 - 2 * k
    across = c + 2 - 4 * x
    diagonal = 3 - c
    peers = (across, diagonal, core)
    tl, il = tok.shape
    tb = 4 * tl
    half = tb // 2
    ib = il // 4
    ic = ib // CHUNKS
    ol = w.shape[1]

    up_ok, down_ok = r < 3, r > 0
    inner, outer = jnp.logical_and(up_ok, down_ok), jnp.logical_or(r == 0, r == 3)

    def tell(sem, to, cond=None):
        when(cond, lambda: pl.semaphore_signal(sem, inc=1, device_id=to, device_id_type=MESH))

    def when(cond, f):
        if cond is None:
            f()
        else:
            pl.when(cond)(f)

    barrier = pltpu.get_barrier_semaphore()
    for q in peers:
        tell(barrier, {"col": q})
    tell(barrier, {"depth": other})
    tell(barrier, {"row": r + 1}, up_ok)
    tell(barrier, {"row": r - 1}, down_ok)
    when(inner, lambda: pl.semaphore_wait(barrier, 6))
    when(outer, lambda: pl.semaphore_wait(barrier, 5))
    tell(come.at[0], {"row": r + 1}, inner)
    tell(come.at[1], {"row": r - 1}, inner)

    def all_in():
        @pl.when(r >= 2)
        def _():
            pl.semaphore_wait(come.at[0], 1)

        @pl.when(r <= 1)
        def _():
            pl.semaphore_wait(come.at[1], 1)

        tell(come.at[2], {"row": r + 1}, r == 2)
        tell(come.at[2], {"row": r - 1}, r == 1)

        @pl.when(outer)
        def _():
            pl.semaphore_wait(come.at[2], 1)

    def send(src, dst, kind, r_sem, to, cond=None):
        copy = pltpu.make_async_remote_copy(
            src_ref=src, dst_ref=dst, send_sem=gone.at[kind], recv_sem=r_sem, device_id=to, device_id_type=MESH
        )
        when(cond, copy.start)

    def local(src, dst, sem, cond=None):
        when(cond, pltpu.make_async_copy(src, dst, sem).start)

    def arrived(ref, sem, cond=None):
        when(cond, pltpu.make_async_copy(ref, ref, sem).wait)

    def at(i, n):
        return pl.ds(pl.multiple_of(i * n, n), n)

    def g_unit(s, h, q):
        return g_all.at[at(s * 2 + h, half), at(place(q), ol)]

    def far_first(depth):
        return depth, 1 - depth

    for h in far_first(d):
        to = 2 * d + h
        mine = to == r
        ours = g.at[at(d, half), at(h, ol)]
        theirs = g.at[at(other, half), at(h, ol)]
        send(theirs, g_unit(r, other, c), PRE, g_z.at[r], {"depth": other}, mine)
        send(theirs, g_mid.at[h], PRE, g_pre.at[h], {"depth": other}, jnp.logical_not(mine))
        local(ours, g_unit(r, d, c), g_z.at[r], mine)
        near = jnp.logical_or(to == r + 1, to == r - 1)
        send(ours, g_unit(r, d, c), Z, g_z.at[r], {"row": to}, near)

    def features(q, j):
        return at(q * CHUNKS + j, ic)

    def send_tokens(j):
        for i, q in enumerate(peers):
            send(
                tok.at[:, features(q, j)], x_all.at[j, at(r * 4 + c, tl)],
                TOK, x_r.at[j], {"col": q},
            )
        local(tok.at[:, features(c, j)], x_all.at[j, at(r * 4 + c, tl)], x_r.at[j])

    def home(q):
        return at((q * CHUNKS + LAST) * 2 + 1, ic // 2)

    def facing(q):
        return q + 2 - 4 * (q // 2)

    def send_home_tokens():
        rows = at(r * 4 + c, tl)
        for i, q in enumerate(peers):
            send(tok.at[:, home(facing(q))], x_home.at[rows], HOME, x_r.at[CHUNKS], {"col": q})
        local(tok.at[:, home(across)], x_home.at[rows], x_r.at[CHUNKS])

    def send_weight(j):
        for i, q in enumerate(peers):
            send(
                w.at[at(q * CHUNKS + j, ic)], w_all.at[j, :, at(place(c), ol)],
                W, w_r.at[j], {"col": q},
            )
        local(w.at[at(c * CHUNKS + j, ic)], w_all.at[j, :, at(place(c), ol)], w_r.at[j])

    for j in range(CHUNKS):
        send_tokens(j)
    send_home_tokens()
    send_weight(0)

    all_in()
    for h in far_first(d):
        to = 2 * d + h
        away = jnp.logical_or(to > r + 1, to < r - 1)
        send(g.at[at(d, half), at(h, ol)], g_unit(r, d, c), Z, g_z.at[r], {"row": to}, away)

    def gathered(j, s, n):
        return x_all.at[j, at(s, n)] if j < CHUNKS else x_home.at[at(s, n)]

    def tokens_on(j, s, direction, cond):
        block = gathered(j, s, tb)
        kind = (TOK_UP if j < CHUNKS else HOME_UP) + direction
        send(block, block, kind, x_z.at[j, s], {"row": r + 1 - 2 * direction}, cond)

    def own_tokens_on(j):
        arrived(gathered(j, r, tb), x_r.at[j])
        tokens_on(j, r, 0, up_ok)
        tokens_on(j, r, 1, down_ok)

    def pass_tokens(j, far):
        below, above = r - far, r + far
        low, high = jnp.maximum(below, 0), jnp.minimum(above, 3)
        has_low, has_high = below >= 0, above <= 3
        arrived(gathered(j, low, tb), x_z.at[j, low], has_low)
        tokens_on(j, low, 0, jnp.logical_and(has_low, up_ok))
        arrived(gathered(j, high, tb), x_z.at[j, high], has_high)
        tokens_on(j, high, 1, jnp.logical_and(has_high, down_ok))

    near = 3 * (1 - r // 2)
    last = 1 + r % 2
    order = [near, 6 - r - near - last, last, r]

    def spread(n):
        s = order[n]
        unit = g_unit(s, d, c)
        arrived(unit, g_z.at[s])
        send(unit, unit, Y, g_y.at[s], {"depth": other})
        if n < 3:
            spread_across(n)

    def spread_across(n):
        s = order[n]
        unit = g_unit(s, d, c)
        send(unit, unit, X, g_x.at[s], {"col": across})

    def crossed(n):
        s = order[n]
        unit = g_unit(s, d, across)
        arrived(unit, g_x.at[s])
        send(unit, unit, Y, g_y.at[s], {"depth": other})

    def to_core(n):
        s = order[n]
        arrived(g_all.at[at(s * 2 + other, half), at(k, 2 * ol)], g_y.at[s])
        slab = g_all.at[at(s, tb), at(k, 2 * ol)]
        send(slab, slab, CORE, g_d.at[s], {"col": core})

    def pass_mid(i):
        h = far_first(other)[i]
        to = 2 * other + h
        go = to != r
        arrived(g_mid.at[h], g_pre.at[h], go)
        send(g_mid.at[h], g_unit(r, d, c), Z, g_z.at[r], {"row": to}, go)

    def from_core(n):
        s = order[n]
        arrived(g_all.at[at(s, tb), at(1 - k, 2 * ol)], g_d.at[s])

    def weight_in(j):
        arrived(w_all.at[j], w_r.at[j])

    def multiply_block(j, s):
        rows = at(s, tb)
        part[j, rows, :] = lax.dot_general(
            g_all[rows, :], w_all[j], last_with_last, preferred_element_type=F32
        )

    def multiply_input(j):
        def body(b, carry):
            multiply_block(j, b)
            return carry

        lax.fori_loop(0, 4, body, None)

    def turn_tokens(j):
        def turn(b, carry):
            x_t[:, at(b, half)] = x_all[j, at(b, half), :].T
            return carry

        lax.fori_loop(0, 8, turn, None)

    def multiply_columns(rows, q):
        return jnp.dot(x_t[rows, :], g_all[:, at(q, ol)], preferred_element_type=F32).astype(BF16)

    def multiply_weight(j):
        turn_tokens(j)

        def body(n, carry):
            gw_out[j, :, at(n, ol)] = multiply_columns(pl.ds(0, ic), n)
            return carry

        lax.fori_loop(0, 4, body, None)
        for i, q in enumerate(peers):
            send(
                gw_out.at[j, :, at(place(q), ol)], gw.at[features(c, j)],
                GW, done.at[1], {"col": q},
            )
        local(gw_out.at[j, :, at(place(c), ol)], gw.at[features(c, j)], done.at[1])

    first, second = pl.ds(0, ic // 2), pl.ds(ic // 2, ic // 2)

    def front(q):
        return at((q * CHUNKS + LAST) * 2, ic // 2)

    def multiply_weight_last():
        turn_tokens(LAST)

        def body(n, carry):
            q = 2 * n + 1 - x
            gw_out[LAST, first, at(q, ol)] = multiply_columns(first, q)
            return carry

        lax.fori_loop(0, 2, body, None)
        for i, q in enumerate((across, diagonal)):
            send(
                gw_out.at[LAST, first, at(place(q), ol)], gw.at[front(c)],
                GW, done.at[1], {"col": q},
            )

        def body(n, carry):
            q = 2 * n + x
            gw_out[LAST, :, at(q, ol)] = multiply_columns(pl.ds(0, ic), q)
            return carry

        lax.fori_loop(0, 2, body, None)
        rows = features(c, LAST)
        send(
            gw_out.at[LAST, :, at(place(core), ol)], gw.at[rows],
            GW, done.at[1], {"col": core},
        )
        local(gw_out.at[LAST, :, at(place(c), ol)], gw.at[rows], done.at[1])

    def multiply_weight_home():
        def turn(b, carry):
            x_t[first, at(b, half)] = x_home[at(b, half), :].T
            return carry

        lax.fori_loop(0, 8, turn, None)

        def body(n, carry):
            gw_out[LAST, second, at(2 * n + 1 - x, ol)] = multiply_columns(first, 2 * n + x)
            return carry

        lax.fori_loop(0, 2, body, None)
        rows = home(across)
        send(
            gw_out.at[LAST, second, at(place(diagonal), ol)], gw.at[rows],
            GW, done.at[1], {"col": core},
        )
        local(gw_out.at[LAST, second, at(place(across), ol)], gw.at[rows], done.at[1])

    step = 64
    scale_rows = pl.ds(tb, GROUP)

    def read_code(buf, i, rows, unit):
        v = buf[i, rows, :].astype(F32)
        size = jnp.log(jnp.abs(v)) + SPAN
        size = size * jnp.concatenate([unit] * (step // GROUP), axis=0)
        return jnp.where(v < 0, -size, size)

    def unit_of(buf, i):
        return buf[i, scale_rows, :].astype(F32) * (0.5 / SPAN)

    def encode(j, b, out, slot, got):
        unit = None if got is None else unit_of(got, slot)

        def total(t):
            value = part[j, pl.ds(pl.multiple_of(b * tb + t * step, step), step), :]
            if got is not None:
                value = value + read_code(got, slot, at(t, step), unit)
            return value

        def first(t, most):
            value = total(t)
            if got is not None:
                part[j, pl.ds(pl.multiple_of(b * tb + t * step, step), step), :] = value
            size = jnp.abs(value)
            for n in range(step // GROUP):
                most = jnp.maximum(most, size[n * GROUP : (n + 1) * GROUP])
            return most

        most = lax.fori_loop(0, tb // step, first, jnp.full((GROUP, ic), TINY, F32))
        scale = (most * 1.01).astype(BF16)
        out[slot, scale_rows, :] = scale
        by = (2 * SPAN) / scale.astype(F32)
        by = jnp.concatenate([by] * (step // GROUP), axis=0)

        def second(t, carry):
            value = part[j, pl.ds(pl.multiple_of(b * tb + t * step, step), step), :]
            code = jnp.exp(jnp.abs(value) * by - SPAN)
            out[slot, at(t, step), :] = jnp.where(value < 0, -code, code).astype(BF16)
            return carry

        lax.fori_loop(0, tb // step, second, None)

    def add_in(j, got, slot):
        unit = unit_of(got, slot)

        def body(t, carry):
            rows = pl.ds(pl.multiple_of(r * tb + t * step, step), step)
            part[j, rows, :] = part[j, rows, :] + read_code(got, slot, at(t, step), unit)
            return carry

        lax.fori_loop(0, tb // step, body, None)

    def ring(j, level, up, which):
        here = level if up else 3 - level
        out, got, kind, r_sem = (ups, upr, UP, up_r) if up else (dns, dnr, DOWN, dn_r)
        toward = {"row": r + 1 if up else r - 1}
        far = [3, 2, 1, 0] if up else [0, 1, 2, 3]
        cond = r == here
        for n in which:
            b = far[n]
            i = j * 3 + (b - 1 if up else b)
            if b == here:

                @pl.when(cond)
                def _():
                    arrived(got.at[i], r_sem.at[i])
                    add_in(j, got, i)

                continue
            copy = pltpu.make_async_remote_copy(
                src_ref=out.at[i], dst_ref=got.at[i], send_sem=gone.at[kind], recv_sem=r_sem.at[i],
                device_id=toward, device_id_type=MESH,
            )

            @pl.when(cond)
            def _():
                if level > 0:
                    arrived(got.at[i], r_sem.at[i])
                encode(j, b, out, i, got if level > 0 else None)
                copy.start()

    def level(j, n, which=None):
        which = range(4 - n if n else 3) if which is None else which
        ring(j, n, True, which)
        ring(j, n, False, which)

    def finish(j, cond):
        @pl.when(cond)
        def _():
            gi_out[j] = part[j, at(r, tb), :].astype(BF16)

        for i, q in enumerate(peers):
            send(
                gi_out.at[j, at(q, tl)], gi.at[:, at(c * CHUNKS + j, ic)],
                GI, done.at[0], {"col": q}, cond,
            )
        local(gi_out.at[j, at(c, tl)], gi.at[:, at(c * CHUNKS + j, ic)], done.at[0], cond)

    def run(name, f, *args):
        with jax.named_scope(name):
            f(*args)

    def mi(j):
        run("w_in%d" % j, weight_in, j)
        run("input%d" % j, multiply_input, j)

    def mw(j):
        run("pass%d_3" % j, pass_tokens, j, 3)
        run("weight%d" % j, multiply_weight if j < LAST else multiply_weight_last, *([j] if j < LAST else []))

    def lv(j, n, which=None):
        run("level%d_%d" % (j, n), level, j, n, which)

    def end(j, cond, name):
        run("end%d_%s" % (j, name), finish, j, cond)

    def block(n):
        run("from_core%d" % n, from_core, n)
        run("block%d" % n, multiply_block, 0, order[n])
        if n < 3:
            run("first%d" % n, level, 0, 0, [n])

    def ps(j, far):
        run("pass%d_%d" % (j, far), pass_tokens, j, far)

    def l0(j, n):
        run("l0_%d%d" % (j, n), level, j, 0, [n])

    def l1(j, n):
        run("l1_%d%d" % (j, n), level, j, 1, [n])

    def l2(j, n):
        run("l2_%d%d" % (j, n), level, j, 2, [n])

    def l3(j):
        run("l3_%d" % j, level, j, 3, [0])
        end(j, outer, "out")

    def some(j, n):
        run("blk%d_%d" % (j, n), multiply_block, j, order[n])

    run("own0", own_tokens_on, 0)
    run("mid0", pass_mid, 0)
    run("spread3", spread, 3)
    run("mid1", pass_mid, 1)
    run("own1", own_tokens_on, 1)
    for n in range(3):
        run("spread%d" % n, spread, n)
    spread_across(3)
    for j in range(1, CHUNKS):
        send_weight(j)
    run("own2", own_tokens_on, 2)
    ps(0, 1)
    run("own3", own_tokens_on, 3)
    run("own4", own_tokens_on, 4)
    run("crossed0", crossed, 0)
    run("crossed1", crossed, 1)
    ps(1, 1)
    run("crossed2", crossed, 2)
    ps(2, 1)
    run("to_core0", to_core, 0)
    run("w_in0", weight_in, 0)
    block(0)
    run("to_core1", to_core, 1)
    run("crossed3", crossed, 3)
    ps(0, 2)
    block(1)
    ps(3, 1)
    ps(4, 1)
    run("to_core2", to_core, 2)
    block(2)
    l1(0, 0)
    run("to_core3", to_core, 3)
    ps(1, 2)
    run("w_in1", weight_in, 1)
    for n in range(3):
        some(1, n)
        l0(1, n)
    block(3)
    some(1, 3)
    l1(0, 1)
    l1(0, 2)
    ps(2, 2)
    mw(0)
    mi(2)
    for n in range(3):
        l0(2, n)
    l1(1, 0)
    l2(0, 0)
    l1(1, 1)
    l2(0, 1)
    end(0, inner, "in")
    l1(1, 2)
    ps(3, 2)
    ps(4, 2)
    mw(1)
    mi(3)
    for n in range(3):
        l0(3, n)
    l3(0)
    l2(1, 0)
    l1(2, 0)
    l2(1, 1)
    end(1, inner, "in")
    mw(2)
    l1(2, 1)
    l2(2, 0)
    l3(1)
    l1(2, 2)
    mw(3)
    l1(3, 0)
    l2(2, 1)
    end(2, inner, "in")
    l3(2)
    l1(3, 1)
    l2(3, 0)
    l1(3, 2)
    l2(3, 1)
    end(3, inner, "in")
    ps(4, 3)
    run("home", multiply_weight_home)
    l3(3)

    def drain():
        def all_gone(kind, ref, cond=None):
            arrived(ref, gone.at[kind], cond)

        def units(n):
            return g_all.at[pl.ds(0, n * half // 4)]

        for kind, n in ((PRE, 2), (Z, 3), (X, 4), (Y, 8), (CORE, 16)):
            all_gone(kind, units(n))
        all_gone(TOK, x_all.at[0, pl.ds(0, 3 * CHUNKS * tl)])
        all_gone(HOME, x_home.at[pl.ds(0, 3 * tl)])
        all_gone(W, w_all.at[pl.ds(0, 3)])
        for n in range(3):
            for at_n, tok_kind, home_kind, kind, ref in (
                (r == n, TOK_UP, HOME_UP, UP, ups), (r == 3 - n, TOK_DOWN, HOME_DOWN, DOWN, dns)
            ):
                all_gone(tok_kind, x_all.at[pl.ds(0, n + 1)], at_n)
                all_gone(home_kind, x_home.at[pl.ds(0, (n + 1) * tb)], at_n)
                all_gone(kind, ref.at[pl.ds(0, (3 - n) * CHUNKS)], at_n)
        all_gone(GI, x_all.at[0, pl.ds(0, 3 * CHUNKS * tl)])
        all_gone(GW, g_all.at[pl.ds(0, (6 * LAST + 5) * ic // 8)])

    def outputs():
        arrived(gi, done.at[0])
        arrived(gw, done.at[1])

    run("drain", drain)
    run("outputs", outputs)


PIECES = 4


def store_kernel(gi_in, gw_in, gi, gw, sem):
    n = gw.shape[0] // PIECES
    copies = [
        pltpu.make_async_copy(gw_in.at[pl.ds(i * n, n)], gw.at[pl.ds(i * n, n)], sem.at[i])
        for i in range(PIECES)
    ] + [pltpu.make_async_copy(gi_in, gi, sem.at[PIECES])]
    for copy in copies:
        copy.start()
    for copy in copies:
        copy.wait()


def store(grad_input, grad_weight):
    anywhere = pl.BlockSpec(memory_space=pl.ANY)
    return pl.pallas_call(
        store_kernel,
        out_shape=(
            jax.ShapeDtypeStruct(grad_input.shape, BF16),
            jax.ShapeDtypeStruct(grad_weight.shape, BF16),
        ),
        in_specs=[anywhere] * 2,
        out_specs=(anywhere, anywhere),
        scratch_shapes=[pltpu.SemaphoreType.DMA((PIECES + 1,))],
        compiler_params=pltpu.CompilerParams(vmem_limit_bytes=2**20),
    )(grad_input, grad_weight)


def per_device_kernel(tokens, weight, grad_output):
    tl, il = tokens.shape
    ol = weight.shape[1]
    tb, ic = 4 * tl, il // (4 * CHUNKS)
    dma = pltpu.SemaphoreType.DMA
    code = pltpu.VMEM((3 * CHUNKS, tb + GROUP, ic), BF16)
    anywhere = pl.BlockSpec(memory_space=pl.ANY)
    return store(*pl.pallas_call(
        kernel,
        out_shape=(
            jax.ShapeDtypeStruct(tokens.shape, BF16),
            jax.ShapeDtypeStruct(weight.shape, BF16),
        ),
        in_specs=[anywhere] * 3,
        out_specs=(anywhere, anywhere),
        scratch_shapes=[
            pltpu.VMEM((4 * tb, 4 * ol), BF16),
            pltpu.VMEM((2, tb // 2, ol), BF16),
            pltpu.VMEM((CHUNKS, 4 * tb, ic), BF16),
            pltpu.VMEM((ic, 4 * tb), BF16),
            pltpu.VMEM((CHUNKS, ic, 4 * ol), BF16),
            pltpu.VMEM((CHUNKS, 4 * tb, ic), F32),
            pltpu.VMEM((CHUNKS, ic, 4 * ol), BF16),
            pltpu.VMEM((CHUNKS, tb, ic), BF16),
            code, code, code, code,
            pltpu.VMEM((4 * tb, ic // 2), BF16), pltpu.SemaphoreType.REGULAR((3,)),
            dma((2,)), dma((4,)), dma((4,)), dma((4,)), dma((4,)), dma((CHUNKS + 1,)), dma((CHUNKS,)),
            dma((CHUNKS + 1, 4)), dma((3 * CHUNKS,)), dma((3 * CHUNKS,)), dma((2,)), dma((16,)),
        ],
        compiler_params=pltpu.CompilerParams(
            collective_id=0, has_side_effects=True, vmem_limit_bytes=46 * 2**20
        ),
    )(*[pltpu.with_memory_space_constraint(a, pltpu.HBM) for a in (tokens, weight, grad_output)]))


def solution(mesh):
    fours_fit = mesh.shape["row"] == 4 and mesh.shape["col"] == 4 and mesh.shape["depth"] == 2
    return jax.shard_map(
        per_device_kernel if fours_fit else per_device_general,
        mesh=mesh,
        in_specs=(
            P(("row", "col"), "depth"),
            P("depth", ("col", "row")),
            P("row", ("col", "depth")),
        ),
        out_specs=(P(("row", "col"), "depth"), P("depth", ("col", "row"))),
        check_vma=False,
    )
```

```python
import jax
import jax.numpy as jnp
from jax import lax
from jax.experimental import pallas as pl
from jax.experimental.pallas import tpu as pltpu
from jax.sharding import PartitionSpec as P

last_with_last = (((1,), (1,)), ((), ()))
first_with_first = (((0,), (0,)), ((), ()))
MESH = pl.DeviceIdType.MESH
PRE, Z, X, Y, CORE, TOK, HOME, W, UP, DOWN, TOK_UP, TOK_DOWN, HOME_UP, HOME_DOWN, UP2, DOWN2, GI, GW = range(18)
CHUNKS = 4
LAST = CHUNKS - 1
GROUP = 16
SPAN = 83.0
TINY = 1e-30
F32, BF16 = jnp.float32, jnp.bfloat16


def input_grads(weight, grad_block):
    weight_block = lax.all_gather(weight, "row", axis=1, tiled=True)
    partial_value = lax.dot_general(
        grad_block, weight_block, last_with_last, preferred_element_type=jnp.float32
    )
    column_slab = lax.psum_scatter(partial_value, "col", scatter_dimension=1, tiled=True).astype(
        jnp.bfloat16
    )
    return lax.all_to_all(column_slab, "col", split_axis=0, concat_axis=1, tiled=True)


def weight_grads(tokens, grad_block):
    partial_value = lax.dot_general(
        lax.all_gather(tokens, "col", axis=0, tiled=True),
        grad_block,
        first_with_first,
        preferred_element_type=jnp.float32,
    )
    return lax.psum_scatter(partial_value, "row", scatter_dimension=1, tiled=True).astype(
        jnp.bfloat16
    )


def per_device_general(tokens, weight, grad_output):
    grad_block = lax.all_gather(grad_output, "depth", axis=1, tiled=True)
    grad_input = input_grads(weight, grad_block)
    grad_weight = weight_grads(tokens, grad_block)
    return (grad_input, grad_weight)


def place(c):
    return 2 * (c % 2) + c // 2


def kernel(
    tok, w, g, gi, gw,
    g_all, g_mid, x_all, x_t, w_all, part, gw_out, gi_out, ups, upr, dns, dnr, ups2, upr2, dns2, dnr2,
    x_home, come, g_pre, g_z, g_x, g_y, g_d, x_r, w_r, x_z, up_r, dn_r, done, gone,
):
    r, c, d = lax.axis_index("row"), lax.axis_index("col"), lax.axis_index("depth")
    k, x = c % 2, c // 2
    other = 1 - d
    core = c + 1 - 2 * k
    across = c + 2 - 4 * x
    diagonal = 3 - c
    peers = (across, diagonal, core)
    tl, il = tok.shape
    tb = 4 * tl
    half = tb // 2
    ib = il // 4
    ic = ib // CHUNKS
    ol = w.shape[1]

    up_ok, down_ok = r < 3, r > 0
    inner, outer = jnp.logical_and(up_ok, down_ok), jnp.logical_or(r == 0, r == 3)

    def tell(sem, to, cond=None):
        when(cond, lambda: pl.semaphore_signal(sem, inc=1, device_id=to, device_id_type=MESH))

    def when(cond, f):
        if cond is None:
            f()
        else:
            pl.when(cond)(f)

    barrier = pltpu.get_barrier_semaphore()
    for q in peers:
        tell(barrier, {"col": q})
    tell(barrier, {"depth": other})
    tell(barrier, {"row": r + 1}, up_ok)
    tell(barrier, {"row": r - 1}, down_ok)
    when(inner, lambda: pl.semaphore_wait(barrier, 6))
    when(outer, lambda: pl.semaphore_wait(barrier, 5))
    tell(come.at[0], {"row": r + 1}, inner)
    tell(come.at[1], {"row": r - 1}, inner)

    def all_in():
        @pl.when(r >= 2)
        def _():
            pl.semaphore_wait(come.at[0], 1)

        @pl.when(r <= 1)
        def _():
            pl.semaphore_wait(come.at[1], 1)

        tell(come.at[2], {"row": r + 1}, r == 2)
        tell(come.at[2], {"row": r - 1}, r == 1)

        @pl.when(outer)
        def _():
            pl.semaphore_wait(come.at[2], 1)

    def send(src, dst, kind, r_sem, to, cond=None):
        copy = pltpu.make_async_remote_copy(
            src_ref=src, dst_ref=dst, send_sem=gone.at[kind], recv_sem=r_sem, device_id=to, device_id_type=MESH
        )
        when(cond, copy.start)

    def local(src, dst, sem, cond=None):
        when(cond, pltpu.make_async_copy(src, dst, sem).start)

    def arrived(ref, sem, cond=None):
        when(cond, pltpu.make_async_copy(ref, ref, sem).wait)

    def at(i, n):
        return pl.ds(pl.multiple_of(i * n, n), n)

    def g_unit(s, h, q):
        return g_all.at[at(s * 2 + h, half), at(place(q), ol)]

    def far_first(depth):
        return depth, 1 - depth

    for h in far_first(d):
        to = 2 * d + h
        mine = to == r
        ours = g.at[at(d, half), at(h, ol)]
        theirs = g.at[at(other, half), at(h, ol)]
        send(theirs, g_unit(r, other, c), PRE, g_z.at[r], {"depth": other}, mine)
        send(theirs, g_mid.at[h], PRE, g_pre.at[h], {"depth": other}, jnp.logical_not(mine))
        local(ours, g_unit(r, d, c), g_z.at[r], mine)
        near = jnp.logical_or(to == r + 1, to == r - 1)
        send(ours, g_unit(r, d, c), Z, g_z.at[r], {"row": to}, near)

    def features(q, j):
        return at(q * CHUNKS + j, ic)

    def send_tokens(j):
        for i, q in enumerate(peers):
            send(
                tok.at[:, features(q, j)], x_all.at[j, at(r * 4 + c, tl)],
                TOK, x_r.at[j], {"col": q},
            )
        local(tok.at[:, features(c, j)], x_all.at[j, at(r * 4 + c, tl)], x_r.at[j])

    def home(q):
        return at((q * CHUNKS + LAST) * 2 + 1, ic // 2)

    def facing(q):
        return q + 2 - 4 * (q // 2)

    def send_home_tokens():
        rows = at(r * 4 + c, tl)
        for i, q in enumerate(peers):
            send(tok.at[:, home(facing(q))], x_home.at[rows], HOME, x_r.at[CHUNKS], {"col": q})
        local(tok.at[:, home(across)], x_home.at[rows], x_r.at[CHUNKS])

    def send_weight(j):
        for i, q in enumerate(peers):
            send(
                w.at[at(q * CHUNKS + j, ic)], w_all.at[j, :, at(place(c), ol)],
                W, w_r.at[j], {"col": q},
            )
        local(w.at[at(c * CHUNKS + j, ic)], w_all.at[j, :, at(place(c), ol)], w_r.at[j])

    for j in range(CHUNKS):
        send_tokens(j)
    send_home_tokens()
    send_weight(0)

    all_in()
    for h in far_first(d):
        to = 2 * d + h
        away = jnp.logical_or(to > r + 1, to < r - 1)
        send(g.at[at(d, half), at(h, ol)], g_unit(r, d, c), Z, g_z.at[r], {"row": to}, away)

    def gathered(j, s, n):
        return x_all.at[j, at(s, n)] if j < CHUNKS else x_home.at[at(s, n)]

    def tokens_on(j, s, direction, cond):
        block = gathered(j, s, tb)
        kind = (TOK_UP if j < CHUNKS else HOME_UP) + direction
        send(block, block, kind, x_z.at[j, s], {"row": r + 1 - 2 * direction}, cond)

    def own_tokens_on(j):
        arrived(gathered(j, r, tb), x_r.at[j])
        tokens_on(j, r, 0, up_ok)
        tokens_on(j, r, 1, down_ok)

    def pass_tokens(j, far):
        below, above = r - far, r + far
        low, high = jnp.maximum(below, 0), jnp.minimum(above, 3)
        has_low, has_high = below >= 0, above <= 3
        arrived(gathered(j, low, tb), x_z.at[j, low], has_low)
        tokens_on(j, low, 0, jnp.logical_and(has_low, up_ok))
        arrived(gathered(j, high, tb), x_z.at[j, high], has_high)
        tokens_on(j, high, 1, jnp.logical_and(has_high, down_ok))

    near = 3 * (1 - r // 2)
    last = 1 + r % 2
    order = [near, 6 - r - near - last, last, r]

    def spread(n):
        s = order[n]
        unit = g_unit(s, d, c)
        arrived(unit, g_z.at[s])
        send(unit, unit, Y, g_y.at[s], {"depth": other})
        if n < 3:
            spread_across(n)

    def spread_across(n):
        s = order[n]
        unit = g_unit(s, d, c)
        send(unit, unit, X, g_x.at[s], {"col": across})

    def crossed(n):
        s = order[n]
        unit = g_unit(s, d, across)
        arrived(unit, g_x.at[s])
        send(unit, unit, Y, g_y.at[s], {"depth": other})

    def to_core(n):
        s = order[n]
        arrived(g_all.at[at(s * 2 + other, half), at(k, 2 * ol)], g_y.at[s])
        slab = g_all.at[at(s, tb), at(k, 2 * ol)]
        send(slab, slab, CORE, g_d.at[s], {"col": core})

    def pass_mid(i):
        h = far_first(other)[i]
        to = 2 * other + h
        go = to != r
        arrived(g_mid.at[h], g_pre.at[h], go)
        send(g_mid.at[h], g_unit(r, d, c), Z, g_z.at[r], {"row": to}, go)

    def from_core(n):
        s = order[n]
        arrived(g_all.at[at(s, tb), at(1 - k, 2 * ol)], g_d.at[s])

    def weight_in(j):
        arrived(w_all.at[j], w_r.at[j])

    def multiply_block(j, s):
        rows = at(s, tb)
        part[j, rows, :] = lax.dot_general(
            g_all[rows, :], w_all[j], last_with_last, preferred_element_type=F32
        )

    def multiply_input(j):
        def body(b, carry):
            multiply_block(j, b)
            return carry

        lax.fori_loop(0, 4, body, None)

    def turn_tokens(j):
        def turn(b, carry):
            x_t[:, at(b, half)] = x_all[j, at(b, half), :].T
            return carry

        lax.fori_loop(0, 8, turn, None)

    def multiply_columns(rows, q):
        return jnp.dot(x_t[rows, :], g_all[:, at(q, ol)], preferred_element_type=F32).astype(BF16)

    def multiply_weight(j):
        turn_tokens(j)

        def body(n, carry):
            gw_out[j, :, at(n, ol)] = multiply_columns(pl.ds(0, ic), n)
            return carry

        lax.fori_loop(0, 4, body, None)
        for i, q in enumerate(peers):
            send(
                gw_out.at[j, :, at(place(q), ol)], gw.at[features(c, j)],
                GW, done.at[1], {"col": q},
            )
        local(gw_out.at[j, :, at(place(c), ol)], gw.at[features(c, j)], done.at[1])

    first, second = pl.ds(0, ic // 2), pl.ds(ic // 2, ic // 2)

    def front(q):
        return at((q * CHUNKS + LAST) * 2, ic // 2)

    def multiply_weight_last():
        turn_tokens(LAST)

        def body(n, carry):
            q = 2 * n + 1 - x
            gw_out[LAST, first, at(q, ol)] = multiply_columns(first, q)
            return carry

        lax.fori_loop(0, 2, body, None)
        for i, q in enumerate((across, diagonal)):
            send(
                gw_out.at[LAST, first, at(place(q), ol)], gw.at[front(c)],
                GW, done.at[1], {"col": q},
            )

        def body(n, carry):
            q = 2 * n + x
            gw_out[LAST, :, at(q, ol)] = multiply_columns(pl.ds(0, ic), q)
            return carry

        lax.fori_loop(0, 2, body, None)
        rows = features(c, LAST)
        send(
            gw_out.at[LAST, :, at(place(core), ol)], gw.at[rows],
            GW, done.at[1], {"col": core},
        )
        local(gw_out.at[LAST, :, at(place(c), ol)], gw.at[rows], done.at[1])

    def multiply_weight_home():
        def turn(b, carry):
            x_t[first, at(b, half)] = x_home[at(b, half), :].T
            return carry

        lax.fori_loop(0, 8, turn, None)

        def body(n, carry):
            gw_out[LAST, second, at(2 * n + 1 - x, ol)] = multiply_columns(first, 2 * n + x)
            return carry

        lax.fori_loop(0, 2, body, None)
        rows = home(across)
        send(
            gw_out.at[LAST, second, at(place(diagonal), ol)], gw.at[rows],
            GW, done.at[1], {"col": core},
        )
        local(gw_out.at[LAST, second, at(place(across), ol)], gw.at[rows], done.at[1])

    step = 64

    def chunk_of(p):
        return min(p, LAST)

    def columns_of(p):
        return pl.ds(0, ic) if p < LAST else at(p - LAST, ic // 2)

    def features_of(p):
        return at(c * CHUNKS + p, ic) if p < LAST else at((c * CHUNKS + LAST) * 2 + p - LAST, ic // 2)

    def part_at(p, b, t):
        return chunk_of(p), pl.ds(pl.multiple_of(b * tb + t * step, step), step), columns_of(p)

    scale_rows = pl.ds(tb, GROUP)

    def read_code(buf, i, rows, unit):
        v = buf[i, rows, :].astype(F32)
        size = jnp.log(jnp.abs(v)) + SPAN
        size = size * jnp.concatenate([unit] * (step // GROUP), axis=0)
        return jnp.where(v < 0, -size, size)

    def unit_of(buf, i):
        return buf[i, scale_rows, :].astype(F32) * (0.5 / SPAN)

    def encode(p, b, out, slot, got):
        unit = None if got is None else unit_of(got, slot)

        def total(t):
            value = part[part_at(p, b, t)]
            if got is not None:
                value = value + read_code(got, slot, at(t, step), unit)
            return value

        def first(t, most):
            value = total(t)
            if got is not None:
                part[part_at(p, b, t)] = value
            size = jnp.abs(value)
            for n in range(step // GROUP):
                most = jnp.maximum(most, size[n * GROUP : (n + 1) * GROUP])
            return most

        most = lax.fori_loop(0, tb // step, first, jnp.full((GROUP, out.shape[-1]), TINY, F32))
        scale = (most * 1.01).astype(BF16)
        out[slot, scale_rows, :] = scale
        by = (2 * SPAN) / scale.astype(F32)
        by = jnp.concatenate([by] * (step // GROUP), axis=0)

        def second(t, carry):
            value = part[part_at(p, b, t)]
            code = jnp.exp(jnp.abs(value) * by - SPAN)
            out[slot, at(t, step), :] = jnp.where(value < 0, -code, code).astype(BF16)
            return carry

        lax.fori_loop(0, tb // step, second, None)

    def add_in(p, got, slot):
        unit = unit_of(got, slot)

        def body(t, carry):
            where = part_at(p, r, t)
            part[where] = part[where] + read_code(got, slot, at(t, step), unit)
            return carry

        lax.fori_loop(0, tb // step, body, None)

    def ring(p, level, up, which):
        here = level if up else 3 - level
        if p < LAST:
            out, got, kind, r_sem = (ups, upr, UP, up_r) if up else (dns, dnr, DOWN, dn_r)
        else:
            out, got, kind, r_sem = (ups2, upr2, UP2, up_r) if up else (dns2, dnr2, DOWN2, dn_r)
        toward = {"row": r + 1 if up else r - 1}
        far = [3, 2, 1, 0] if up else [0, 1, 2, 3]
        cond = r == here
        for n in which:
            b = far[n]
            m = p * 3 + (b - 1 if up else b)
            i = m if p < LAST else m - 3 * LAST
            if b == here:

                @pl.when(cond)
                def _():
                    arrived(got.at[i], r_sem.at[m])
                    add_in(p, got, i)

                continue
            copy = pltpu.make_async_remote_copy(
                src_ref=out.at[i], dst_ref=got.at[i], send_sem=gone.at[kind], recv_sem=r_sem.at[m],
                device_id=toward, device_id_type=MESH,
            )

            @pl.when(cond)
            def _():
                if level > 0:
                    arrived(got.at[i], r_sem.at[m])
                encode(p, b, out, i, got if level > 0 else None)
                copy.start()

    def level(p, n, which=None):
        which = range(4 - n if n else 3) if which is None else which
        ring(p, n, True, which)
        ring(p, n, False, which)

    def finish(p, cond):
        j, columns = chunk_of(p), columns_of(p)

        @pl.when(cond)
        def _():
            gi_out[j, :, columns] = part[j, at(r, tb), columns].astype(BF16)

        for q in peers:
            send(
                gi_out.at[j, at(q, tl), columns], gi.at[:, features_of(p)],
                GI, done.at[0], {"col": q}, cond,
            )
        local(gi_out.at[j, at(c, tl), columns], gi.at[:, features_of(p)], done.at[0], cond)

    def run(name, f, *args):
        with jax.named_scope(name):
            f(*args)

    def mi(j):
        run("w_in%d" % j, weight_in, j)
        run("input%d" % j, multiply_input, j)

    def mw(j):
        run("pass%d_3" % j, pass_tokens, j, 3)
        run("weight%d" % j, multiply_weight if j < LAST else multiply_weight_last, *([j] if j < LAST else []))

    def lv(j, n, which=None):
        run("level%d_%d" % (j, n), level, j, n, which)

    def end(j, cond, name):
        run("end%d_%s" % (j, name), finish, j, cond)

    def block(n):
        run("from_core%d" % n, from_core, n)
        run("block%d" % n, multiply_block, 0, order[n])
        if n < 3:
            run("first%d" % n, level, 0, 0, [n])

    def ps(j, far):
        run("pass%d_%d" % (j, far), pass_tokens, j, far)

    def l0(j, n):
        run("l0_%d%d" % (j, n), level, j, 0, [n])

    def l1(j, n):
        run("l1_%d%d" % (j, n), level, j, 1, [n])

    def l2(j, n):
        run("l2_%d%d" % (j, n), level, j, 2, [n])

    def l3(j):
        run("l3_%d" % j, level, j, 3, [0])
        end(j, outer, "out")

    def some(j, n):
        run("blk%d_%d" % (j, n), multiply_block, j, order[n])

    run("own0", own_tokens_on, 0)
    run("mid0", pass_mid, 0)
    run("spread3", spread, 3)
    run("mid1", pass_mid, 1)
    run("own1", own_tokens_on, 1)
    for n in range(3):
        run("spread%d" % n, spread, n)
    spread_across(3)
    for j in range(1, CHUNKS):
        send_weight(j)
    run("own2", own_tokens_on, 2)
    ps(0, 1)
    run("own3", own_tokens_on, 3)
    run("own4", own_tokens_on, 4)
    run("crossed0", crossed, 0)
    run("crossed1", crossed, 1)
    ps(1, 1)
    run("crossed2", crossed, 2)
    ps(2, 1)
    run("to_core0", to_core, 0)
    run("w_in0", weight_in, 0)
    block(0)
    run("to_core1", to_core, 1)
    run("crossed3", crossed, 3)
    ps(0, 2)
    block(1)
    ps(3, 1)
    ps(4, 1)
    run("to_core2", to_core, 2)
    block(2)
    l1(0, 0)
    run("to_core3", to_core, 3)
    ps(1, 2)
    run("w_in1", weight_in, 1)
    for n in range(3):
        some(1, n)
        l0(1, n)
    block(3)
    some(1, 3)
    l1(0, 1)
    l1(0, 2)
    ps(2, 2)
    mw(0)
    mi(2)
    for n in range(3):
        l0(2, n)
    l1(1, 0)
    l2(0, 0)
    l1(1, 1)
    l2(0, 1)
    end(0, inner, "in")
    l1(1, 2)
    ps(3, 2)
    ps(4, 2)
    mw(1)
    mi(3)
    for p in (LAST, LAST + 1):
        for n in range(3):
            l0(p, n)
    l3(0)
    l2(1, 0)
    l1(2, 0)
    l2(1, 1)
    end(1, inner, "in")
    mw(2)
    l1(2, 1)
    l2(2, 0)
    l3(1)
    l1(2, 2)
    mw(3)
    l1(3, 0)
    l2(2, 1)
    end(2, inner, "in")
    l3(2)
    l1(3, 1)
    l2(3, 0)
    l1(3, 2)
    l1(4, 0)
    l2(3, 1)
    end(3, inner, "in")
    l1(4, 1)
    l3(3)
    l2(4, 0)
    l1(4, 2)
    l2(4, 1)
    end(4, inner, "in")
    ps(4, 3)
    run("home", multiply_weight_home)
    l3(4)


    def drain():
        def all_gone(kind, ref, cond=None):
            arrived(ref, gone.at[kind], cond)

        def units(n):
            return g_all.at[pl.ds(0, n * half // 4)]

        for kind, n in ((PRE, 2), (Z, 3), (X, 4), (Y, 8), (CORE, 16)):
            all_gone(kind, units(n))
        all_gone(TOK, x_all.at[0, pl.ds(0, 3 * CHUNKS * tl)])
        all_gone(HOME, x_home.at[pl.ds(0, 3 * tl)])
        all_gone(W, w_all.at[pl.ds(0, 3)])
        for n in range(3):
            for at_n, tok_kind, home_kind, kind, ref, kind2, ref2 in (
                (r == n, TOK_UP, HOME_UP, UP, ups, UP2, ups2),
                (r == 3 - n, TOK_DOWN, HOME_DOWN, DOWN, dns, DOWN2, dns2),
            ):
                all_gone(tok_kind, x_all.at[pl.ds(0, n + 1)], at_n)
                all_gone(home_kind, x_home.at[pl.ds(0, (n + 1) * tb)], at_n)
                all_gone(kind, ref.at[pl.ds(0, (3 - n) * LAST)], at_n)
                all_gone(kind2, ref2.at[pl.ds(0, (3 - n) * 2)], at_n)
        all_gone(GI, x_all.at[0, pl.ds(0, 3 * CHUNKS * tl)])
        all_gone(GW, g_all.at[pl.ds(0, (6 * LAST + 5) * ic // 8)])

    def outputs():
        arrived(gi, done.at[0])
        arrived(gw, done.at[1])

    run("drain", drain)
    run("outputs", outputs)


PIECES = 4


def store_kernel(gi_in, gw_in, gi, gw, sem):
    n = gw.shape[0] // PIECES
    copies = [
        pltpu.make_async_copy(gw_in.at[pl.ds(i * n, n)], gw.at[pl.ds(i * n, n)], sem.at[i])
        for i in range(PIECES)
    ] + [pltpu.make_async_copy(gi_in, gi, sem.at[PIECES])]
    for copy in copies:
        copy.start()
    for copy in copies:
        copy.wait()


def store(grad_input, grad_weight):
    anywhere = pl.BlockSpec(memory_space=pl.ANY)
    return pl.pallas_call(
        store_kernel,
        out_shape=(
            jax.ShapeDtypeStruct(grad_input.shape, BF16),
            jax.ShapeDtypeStruct(grad_weight.shape, BF16),
        ),
        in_specs=[anywhere] * 2,
        out_specs=(anywhere, anywhere),
        scratch_shapes=[pltpu.SemaphoreType.DMA((PIECES + 1,))],
        compiler_params=pltpu.CompilerParams(vmem_limit_bytes=2**20),
    )(grad_input, grad_weight)


def per_device_kernel(tokens, weight, grad_output):
    tl, il = tokens.shape
    ol = weight.shape[1]
    tb, ic = 4 * tl, il // (4 * CHUNKS)
    dma = pltpu.SemaphoreType.DMA
    code = pltpu.VMEM((3 * LAST, tb + GROUP, ic), BF16)
    code2 = pltpu.VMEM((6, tb + GROUP, ic // 2), BF16)
    anywhere = pl.BlockSpec(memory_space=pl.ANY)
    return store(*pl.pallas_call(
        kernel,
        out_shape=(
            jax.ShapeDtypeStruct(tokens.shape, BF16),
            jax.ShapeDtypeStruct(weight.shape, BF16),
        ),
        in_specs=[anywhere] * 3,
        out_specs=(anywhere, anywhere),
        scratch_shapes=[
            pltpu.VMEM((4 * tb, 4 * ol), BF16),
            pltpu.VMEM((2, tb // 2, ol), BF16),
            pltpu.VMEM((CHUNKS, 4 * tb, ic), BF16),
            pltpu.VMEM((ic, 4 * tb), BF16),
            pltpu.VMEM((CHUNKS, ic, 4 * ol), BF16),
            pltpu.VMEM((CHUNKS, 4 * tb, ic), F32),
            pltpu.VMEM((CHUNKS, ic, 4 * ol), BF16),
            pltpu.VMEM((CHUNKS, tb, ic), BF16),
            code, code, code, code, code2, code2, code2, code2,
            pltpu.VMEM((4 * tb, ic // 2), BF16), pltpu.SemaphoreType.REGULAR((3,)),
            dma((2,)), dma((4,)), dma((4,)), dma((4,)), dma((4,)), dma((CHUNKS + 1,)), dma((CHUNKS,)),
            dma((CHUNKS + 1, 4)), dma((3 * CHUNKS + 3,)), dma((3 * CHUNKS + 3,)), dma((2,)), dma((18,)),
        ],
        compiler_params=pltpu.CompilerParams(
            collective_id=0, has_side_effects=True, vmem_limit_bytes=46 * 2**20
        ),
    )(*[pltpu.with_memory_space_constraint(a, pltpu.HBM) for a in (tokens, weight, grad_output)]))


def solution(mesh):
    fours_fit = mesh.shape["row"] == 4 and mesh.shape["col"] == 4 and mesh.shape["depth"] == 2
    return jax.shard_map(
        per_device_kernel if fours_fit else per_device_general,
        mesh=mesh,
        in_specs=(
            P(("row", "col"), "depth"),
            P("depth", ("col", "row")),
            P("row", ("col", "depth")),
        ),
        out_specs=(P(("row", "col"), "depth"), P("depth", ("col", "row"))),
        check_vma=False,
    )
```

```python
import jax
import jax.numpy as jnp
from jax import lax
from jax.experimental import pallas as pl
from jax.experimental.pallas import tpu as pltpu
from jax.sharding import PartitionSpec as P

last_with_last = (((1,), (1,)), ((), ()))
first_with_first = (((0,), (0,)), ((), ()))
MESH = pl.DeviceIdType.MESH
PRE, Z, X, Y, CORE, TOK, HOME, W, UP, DOWN, TOK_UP, TOK_DOWN, HOME_UP, HOME_DOWN, UP2, DOWN2, GI, GW = range(18)
CHUNKS = 4
LAST = CHUNKS - 1
GROUP = 16
SPAN = 83.0
TINY = 1e-30
F32, BF16 = jnp.float32, jnp.bfloat16


def input_grads(weight, grad_block):
    weight_block = lax.all_gather(weight, "row", axis=1, tiled=True)
    partial_value = lax.dot_general(
        grad_block, weight_block, last_with_last, preferred_element_type=jnp.float32
    )
    column_slab = lax.psum_scatter(partial_value, "col", scatter_dimension=1, tiled=True).astype(
        jnp.bfloat16
    )
    return lax.all_to_all(column_slab, "col", split_axis=0, concat_axis=1, tiled=True)


def weight_grads(tokens, grad_block):
    partial_value = lax.dot_general(
        lax.all_gather(tokens, "col", axis=0, tiled=True),
        grad_block,
        first_with_first,
        preferred_element_type=jnp.float32,
    )
    return lax.psum_scatter(partial_value, "row", scatter_dimension=1, tiled=True).astype(
        jnp.bfloat16
    )


def per_device_general(tokens, weight, grad_output):
    grad_block = lax.all_gather(grad_output, "depth", axis=1, tiled=True)
    grad_input = input_grads(weight, grad_block)
    grad_weight = weight_grads(tokens, grad_block)
    return (grad_input, grad_weight)


def place(c):
    return 2 * (c % 2) + c // 2


def kernel(
    tok, w, g, gi, gw,
    g_all, g_mid, x_all, x_t, w_all, part, gw_out, gi_out, ups, upr, dns, dnr, ups2, upr2, dns2, dnr2,
    x_home, come, g_pre, g_z, g_x, g_y, g_d, x_r, w_r, x_z, up_r, dn_r, done, gone,
):
    r, c, d = lax.axis_index("row"), lax.axis_index("col"), lax.axis_index("depth")
    k, x = c % 2, c // 2
    other = 1 - d
    core = c + 1 - 2 * k
    across = c + 2 - 4 * x
    diagonal = 3 - c
    peers = (across, diagonal, core)
    tl, il = tok.shape
    tb = 4 * tl
    half = tb // 2
    ib = il // 4
    ic = ib // CHUNKS
    ol = w.shape[1]

    up_ok, down_ok = r < 3, r > 0
    inner, outer = jnp.logical_and(up_ok, down_ok), jnp.logical_or(r == 0, r == 3)

    def tell(sem, to, cond=None):
        when(cond, lambda: pl.semaphore_signal(sem, inc=1, device_id=to, device_id_type=MESH))

    def when(cond, f):
        if cond is None:
            f()
        else:
            pl.when(cond)(f)

    barrier = pltpu.get_barrier_semaphore()
    for q in peers:
        tell(barrier, {"col": q})
    tell(barrier, {"depth": other})
    tell(barrier, {"row": r + 1}, up_ok)
    tell(barrier, {"row": r - 1}, down_ok)
    when(inner, lambda: pl.semaphore_wait(barrier, 6))
    when(outer, lambda: pl.semaphore_wait(barrier, 5))
    tell(come.at[0], {"row": r + 1}, inner)
    tell(come.at[1], {"row": r - 1}, inner)

    def all_in():
        @pl.when(r >= 2)
        def _():
            pl.semaphore_wait(come.at[0], 1)

        @pl.when(r <= 1)
        def _():
            pl.semaphore_wait(come.at[1], 1)

        tell(come.at[2], {"row": r + 1}, r == 2)
        tell(come.at[2], {"row": r - 1}, r == 1)

        @pl.when(outer)
        def _():
            pl.semaphore_wait(come.at[2], 1)

    def send(src, dst, kind, r_sem, to, cond=None):
        copy = pltpu.make_async_remote_copy(
            src_ref=src, dst_ref=dst, send_sem=gone.at[kind], recv_sem=r_sem, device_id=to, device_id_type=MESH
        )
        when(cond, copy.start)

    def local(src, dst, sem, cond=None):
        when(cond, pltpu.make_async_copy(src, dst, sem).start)

    def arrived(ref, sem, cond=None):
        when(cond, pltpu.make_async_copy(ref, ref, sem).wait)

    def at(i, n):
        return pl.ds(pl.multiple_of(i * n, n), n)

    def g_unit(s, h, q):
        return g_all.at[at(s * 2 + h, half), at(place(q), ol)]

    def far_first(depth):
        return depth, 1 - depth

    for h in far_first(d):
        to = 2 * d + h
        mine = to == r
        ours = g.at[at(d, half), at(h, ol)]
        theirs = g.at[at(other, half), at(h, ol)]
        send(theirs, g_unit(r, other, c), PRE, g_z.at[r], {"depth": other}, mine)
        send(theirs, g_mid.at[h], PRE, g_pre.at[h], {"depth": other}, jnp.logical_not(mine))
        local(ours, g_unit(r, d, c), g_z.at[r], mine)
        near = jnp.logical_or(to == r + 1, to == r - 1)
        send(ours, g_unit(r, d, c), Z, g_z.at[r], {"row": to}, near)

    def features(q, j):
        return at(q * CHUNKS + j, ic)

    def send_tokens(j):
        for i, q in enumerate(peers):
            send(
                tok.at[:, features(q, j)], x_all.at[j, at(r * 4 + c, tl)],
                TOK, x_r.at[j], {"col": q},
            )
        local(tok.at[:, features(c, j)], x_all.at[j, at(r * 4 + c, tl)], x_r.at[j])

    def home(q):
        return at((q * CHUNKS + LAST) * 2 + 1, ic // 2)

    def facing(q):
        return q + 2 - 4 * (q // 2)

    def send_home_tokens():
        rows = at(r * 4 + c, tl)
        for i, q in enumerate(peers):
            send(tok.at[:, home(facing(q))], x_home.at[rows], HOME, x_r.at[CHUNKS], {"col": q})
        local(tok.at[:, home(across)], x_home.at[rows], x_r.at[CHUNKS])

    def send_weight(j):
        for i, q in enumerate(peers):
            send(
                w.at[at(q * CHUNKS + j, ic)], w_all.at[j, :, at(place(c), ol)],
                W, w_r.at[j], {"col": q},
            )
        local(w.at[at(c * CHUNKS + j, ic)], w_all.at[j, :, at(place(c), ol)], w_r.at[j])

    for j in range(CHUNKS):
        send_tokens(j)
    send_home_tokens()
    send_weight(0)

    all_in()
    for h in far_first(d):
        to = 2 * d + h
        away = jnp.logical_or(to > r + 1, to < r - 1)
        send(g.at[at(d, half), at(h, ol)], g_unit(r, d, c), Z, g_z.at[r], {"row": to}, away)

    def gathered(j, s, n):
        return x_all.at[j, at(s, n)] if j < CHUNKS else x_home.at[at(s, n)]

    def tokens_on(j, s, direction, cond):
        block = gathered(j, s, tb)
        kind = (TOK_UP if j < CHUNKS else HOME_UP) + direction
        send(block, block, kind, x_z.at[j, s], {"row": r + 1 - 2 * direction}, cond)

    def own_tokens_on(j):
        arrived(gathered(j, r, tb), x_r.at[j])
        tokens_on(j, r, 0, up_ok)
        tokens_on(j, r, 1, down_ok)

    def pass_tokens(j, far):
        below, above = r - far, r + far
        low, high = jnp.maximum(below, 0), jnp.minimum(above, 3)
        has_low, has_high = below >= 0, above <= 3
        arrived(gathered(j, low, tb), x_z.at[j, low], has_low)
        tokens_on(j, low, 0, jnp.logical_and(has_low, up_ok))
        arrived(gathered(j, high, tb), x_z.at[j, high], has_high)
        tokens_on(j, high, 1, jnp.logical_and(has_high, down_ok))

    near = 3 * (1 - r // 2)
    last = 1 + r % 2
    order = [near, 6 - r - near - last, last, r]

    def landed(n):
        s = order[n]
        arrived(g_unit(s, d, c), g_z.at[s])

    def spread_over(n):
        s = order[n]
        unit = g_unit(s, d, c)
        send(unit, unit, Y, g_y.at[s], {"depth": other})

    def spread_across(n):
        s = order[n]
        unit = g_unit(s, d, c)
        send(unit, unit, X, g_x.at[s], {"col": across})

    def spread(n):
        landed(n)
        spread_over(n)
        if n < 3:
            spread_across(n)

    def crossed(n):
        s = order[n]
        unit = g_unit(s, d, across)
        arrived(unit, g_x.at[s])
        send(unit, unit, Y, g_y.at[s], {"depth": other})

    def to_core(n):
        s = order[n]
        arrived(g_all.at[at(s * 2 + other, half), at(k, 2 * ol)], g_y.at[s])
        slab = g_all.at[at(s, tb), at(k, 2 * ol)]
        send(slab, slab, CORE, g_d.at[s], {"col": core})

    def pass_mid(i):
        h = far_first(other)[i]
        to = 2 * other + h
        go = to != r
        arrived(g_mid.at[h], g_pre.at[h], go)
        send(g_mid.at[h], g_unit(r, d, c), Z, g_z.at[r], {"row": to}, go)

    def from_core(n):
        s = order[n]
        arrived(g_all.at[at(s, tb), at(1 - k, 2 * ol)], g_d.at[s])

    def weight_in(j):
        arrived(w_all.at[j], w_r.at[j])

    def multiply_block(j, s):
        rows = at(s, tb)
        part[j, rows, :] = lax.dot_general(
            g_all[rows, :], w_all[j], last_with_last, preferred_element_type=F32
        )

    def multiply_input(j):
        def body(b, carry):
            multiply_block(j, b)
            return carry

        lax.fori_loop(0, 4, body, None)

    def turn_tokens(j):
        def turn(b, carry):
            x_t[:, at(b, half)] = x_all[j, at(b, half), :].T
            return carry

        lax.fori_loop(0, 8, turn, None)

    def multiply_columns(rows, q):
        return jnp.dot(x_t[rows, :], g_all[:, at(q, ol)], preferred_element_type=F32).astype(BF16)

    def multiply_weight(j):
        turn_tokens(j)

        def body(n, carry):
            gw_out[j, :, at(n, ol)] = multiply_columns(pl.ds(0, ic), n)
            return carry

        lax.fori_loop(0, 4, body, None)
        for i, q in enumerate(peers):
            send(
                gw_out.at[j, :, at(place(q), ol)], gw.at[features(c, j)],
                GW, done.at[1], {"col": q},
            )
        local(gw_out.at[j, :, at(place(c), ol)], gw.at[features(c, j)], done.at[1])

    first, second = pl.ds(0, ic // 2), pl.ds(ic // 2, ic // 2)

    def front(q):
        return at((q * CHUNKS + LAST) * 2, ic // 2)

    def multiply_weight_last():
        turn_tokens(LAST)

        def body(n, carry):
            q = 2 * n + 1 - x
            gw_out[LAST, first, at(q, ol)] = multiply_columns(first, q)
            return carry

        lax.fori_loop(0, 2, body, None)
        for i, q in enumerate((across, diagonal)):
            send(
                gw_out.at[LAST, first, at(place(q), ol)], gw.at[front(c)],
                GW, done.at[1], {"col": q},
            )

        def body(n, carry):
            q = 2 * n + x
            gw_out[LAST, :, at(q, ol)] = multiply_columns(pl.ds(0, ic), q)
            return carry

        lax.fori_loop(0, 2, body, None)
        rows = features(c, LAST)
        send(
            gw_out.at[LAST, :, at(place(core), ol)], gw.at[rows],
            GW, done.at[1], {"col": core},
        )
        local(gw_out.at[LAST, :, at(place(c), ol)], gw.at[rows], done.at[1])

    def multiply_weight_home():
        def turn(b, carry):
            x_t[first, at(b, half)] = x_home[at(b, half), :].T
            return carry

        lax.fori_loop(0, 8, turn, None)

        def body(n, carry):
            gw_out[LAST, second, at(2 * n + 1 - x, ol)] = multiply_columns(first, 2 * n + x)
            return carry

        lax.fori_loop(0, 2, body, None)
        rows = home(across)
        send(
            gw_out.at[LAST, second, at(place(diagonal), ol)], gw.at[rows],
            GW, done.at[1], {"col": core},
        )
        local(gw_out.at[LAST, second, at(place(across), ol)], gw.at[rows], done.at[1])

    step = 64

    def chunk_of(p):
        return min(p, LAST)

    def columns_of(p):
        return pl.ds(0, ic) if p < LAST else at(p - LAST, ic // 2)

    def features_of(p):
        return at(c * CHUNKS + p, ic) if p < LAST else at((c * CHUNKS + LAST) * 2 + p - LAST, ic // 2)

    def part_at(p, b, t):
        return chunk_of(p), pl.ds(pl.multiple_of(b * tb + t * step, step), step), columns_of(p)

    scale_rows = pl.ds(tb, GROUP)

    def read_code(buf, i, rows, unit):
        v = buf[i, rows, :].astype(F32)
        size = jnp.log(jnp.abs(v)) + SPAN
        size = size * jnp.concatenate([unit] * (step // GROUP), axis=0)
        return jnp.where(v < 0, -size, size)

    def unit_of(buf, i):
        return buf[i, scale_rows, :].astype(F32) * (0.5 / SPAN)

    def encode(p, b, out, slot, got):
        unit = None if got is None else unit_of(got, slot)

        def total(t):
            value = part[part_at(p, b, t)]
            if got is not None:
                value = value + read_code(got, slot, at(t, step), unit)
            return value

        def first(t, most):
            value = total(t)
            if got is not None:
                part[part_at(p, b, t)] = value
            size = jnp.abs(value)
            for n in range(step // GROUP):
                most = jnp.maximum(most, size[n * GROUP : (n + 1) * GROUP])
            return most

        most = lax.fori_loop(0, tb // step, first, jnp.full((GROUP, out.shape[-1]), TINY, F32))
        scale = (most * 1.01).astype(BF16)
        out[slot, scale_rows, :] = scale
        by = (2 * SPAN) / scale.astype(F32)
        by = jnp.concatenate([by] * (step // GROUP), axis=0)

        def second(t, carry):
            value = part[part_at(p, b, t)]
            code = jnp.exp(jnp.abs(value) * by - SPAN)
            out[slot, at(t, step), :] = jnp.where(value < 0, -code, code).astype(BF16)
            return carry

        lax.fori_loop(0, tb // step, second, None)

    def add_in(p, got, slot):
        unit = unit_of(got, slot)

        def body(t, carry):
            where = part_at(p, r, t)
            part[where] = part[where] + read_code(got, slot, at(t, step), unit)
            return carry

        lax.fori_loop(0, tb // step, body, None)

    def ring(p, level, up, which):
        here = level if up else 3 - level
        if p < LAST:
            out, got, kind, r_sem = (ups, upr, UP, up_r) if up else (dns, dnr, DOWN, dn_r)
        else:
            out, got, kind, r_sem = (ups2, upr2, UP2, up_r) if up else (dns2, dnr2, DOWN2, dn_r)
        toward = {"row": r + 1 if up else r - 1}
        far = [3, 2, 1, 0] if up else [0, 1, 2, 3]
        cond = r == here
        for n in which:
            b = far[n]
            m = p * 3 + (b - 1 if up else b)
            i = m if p < LAST else m - 3 * LAST
            if b == here:

                @pl.when(cond)
                def _():
                    arrived(got.at[i], r_sem.at[m])
                    add_in(p, got, i)

                continue
            copy = pltpu.make_async_remote_copy(
                src_ref=out.at[i], dst_ref=got.at[i], send_sem=gone.at[kind], recv_sem=r_sem.at[m],
                device_id=toward, device_id_type=MESH,
            )

            @pl.when(cond)
            def _():
                if level > 0:
                    arrived(got.at[i], r_sem.at[m])
                encode(p, b, out, i, got if level > 0 else None)
                copy.start()

    def level(p, n, which=None):
        which = range(4 - n if n else 3) if which is None else which
        ring(p, n, True, which)
        ring(p, n, False, which)

    def finish(p, cond):
        j, columns = chunk_of(p), columns_of(p)

        @pl.when(cond)
        def _():
            gi_out[j, :, columns] = part[j, at(r, tb), columns].astype(BF16)

        for q in peers:
            send(
                gi_out.at[j, at(q, tl), columns], gi.at[:, features_of(p)],
                GI, done.at[0], {"col": q}, cond,
            )
        local(gi_out.at[j, at(c, tl), columns], gi.at[:, features_of(p)], done.at[0], cond)

    def run(name, f, *args):
        with jax.named_scope(name):
            f(*args)

    def mi(j):
        run("w_in%d" % j, weight_in, j)
        run("input%d" % j, multiply_input, j)

    def mw(j, cond=None):
        if cond is not inner:
            run("pass%d_3" % j, pass_tokens, j, 3)
        if cond is not None:
            pl.when(cond)(lambda: run("weight%d" % j, multiply_weight, j))
            return
        run("weight%d" % j, multiply_weight if j < LAST else multiply_weight_last, *([j] if j < LAST else []))

    def lv(j, n, which=None):
        run("level%d_%d" % (j, n), level, j, n, which)

    def end(j, cond, name):
        run("end%d_%s" % (j, name), finish, j, cond)

    def block(n):
        run("from_core%d" % n, from_core, n)
        run("block%d" % n, multiply_block, 0, order[n])
        if n < 3:
            run("first%d" % n, level, 0, 0, [n])

    def ps(j, far):
        run("pass%d_%d" % (j, far), pass_tokens, j, far)

    def l0(j, n):
        run("l0_%d%d" % (j, n), level, j, 0, [n])

    def l1(j, n):
        run("l1_%d%d" % (j, n), level, j, 1, [n])

    def l2(j, n):
        run("l2_%d%d" % (j, n), level, j, 2, [n])

    def l3(j):
        run("l3_%d" % j, level, j, 3, [0])
        end(j, outer, "out")

    def some(j, n):
        run("blk%d_%d" % (j, n), multiply_block, j, order[n])

    run("own0", own_tokens_on, 0)
    run("mid0", pass_mid, 0)
    run("spread3", spread, 3)
    run("mid1", pass_mid, 1)
    run("own1", own_tokens_on, 1)
    run("spread0", spread, 0)
    run("spread1", spread, 1)
    run("landed2", landed, 2)
    spread_across(2)
    spread_across(3)
    for j in range(1, CHUNKS):
        send_weight(j)
    run("own2", own_tokens_on, 2)
    ps(0, 1)
    run("own3", own_tokens_on, 3)
    run("own4", own_tokens_on, 4)
    run("crossed0", crossed, 0)
    spread_over(2)
    run("crossed1", crossed, 1)
    ps(1, 1)
    run("crossed2", crossed, 2)
    ps(2, 1)
    run("to_core0", to_core, 0)
    run("w_in0", weight_in, 0)
    block(0)
    run("to_core1", to_core, 1)
    run("crossed3", crossed, 3)
    ps(0, 2)
    block(1)
    ps(3, 1)
    ps(4, 1)
    run("to_core2", to_core, 2)
    block(2)
    l1(0, 0)
    run("to_core3", to_core, 3)
    ps(1, 2)
    run("w_in1", weight_in, 1)
    for n in range(3):
        some(1, n)
        l0(1, n)
    block(3)
    some(1, 3)
    l1(0, 1)
    l1(0, 2)
    ps(2, 2)
    mw(0)
    mi(2)
    for n in range(3):
        l0(2, n)
    l1(1, 0)
    mw(1, inner)
    l2(0, 0)
    l1(1, 1)
    l2(0, 1)
    end(0, inner, "in")
    l1(1, 2)
    ps(3, 2)
    ps(4, 2)
    mw(1, outer)
    mi(3)
    for p in (LAST, LAST + 1):
        for n in range(3):
            l0(p, n)
    l3(0)
    l2(1, 0)
    l1(2, 0)
    l2(1, 1)
    end(1, inner, "in")
    mw(2)
    l1(2, 1)
    l2(2, 0)
    l3(1)
    l1(2, 2)
    mw(3)
    l1(3, 0)
    l2(2, 1)
    end(2, inner, "in")
    l3(2)
    l1(3, 1)
    l2(3, 0)
    l1(3, 2)
    l1(4, 0)
    l2(3, 1)
    end(3, inner, "in")
    l1(4, 1)
    l3(3)
    l2(4, 0)
    l1(4, 2)
    l2(4, 1)
    end(4, inner, "in")
    ps(4, 3)
    run("home", multiply_weight_home)
    l3(4)


    def drain():
        def all_gone(kind, ref, cond=None):
            arrived(ref, gone.at[kind], cond)

        def units(n):
            return g_all.at[pl.ds(0, n * half // 4)]

        for kind, n in ((PRE, 2), (Z, 3), (X, 4), (Y, 8), (CORE, 16)):
            all_gone(kind, units(n))
        all_gone(TOK, x_all.at[0, pl.ds(0, 3 * CHUNKS * tl)])
        all_gone(HOME, x_home.at[pl.ds(0, 3 * tl)])
        all_gone(W, w_all.at[pl.ds(0, 3)])
        for n in range(3):
            for at_n, tok_kind, home_kind, kind, ref, kind2, ref2 in (
                (r == n, TOK_UP, HOME_UP, UP, ups, UP2, ups2),
                (r == 3 - n, TOK_DOWN, HOME_DOWN, DOWN, dns, DOWN2, dns2),
            ):
                all_gone(tok_kind, x_all.at[pl.ds(0, n + 1)], at_n)
                all_gone(home_kind, x_home.at[pl.ds(0, (n + 1) * tb)], at_n)
                all_gone(kind, ref.at[pl.ds(0, (3 - n) * LAST)], at_n)
                all_gone(kind2, ref2.at[pl.ds(0, (3 - n) * 2)], at_n)
        all_gone(GI, x_all.at[0, pl.ds(0, 3 * CHUNKS * tl)])
        all_gone(GW, g_all.at[pl.ds(0, (6 * LAST + 5) * ic // 8)])

    def outputs():
        arrived(gi, done.at[0])
        arrived(gw, done.at[1])

    run("drain", drain)
    run("outputs", outputs)


PIECES = 4


def store_kernel(gi_in, gw_in, gi, gw, sem):
    n = gw.shape[0] // PIECES
    copies = [
        pltpu.make_async_copy(gw_in.at[pl.ds(i * n, n)], gw.at[pl.ds(i * n, n)], sem.at[i])
        for i in range(PIECES)
    ] + [pltpu.make_async_copy(gi_in, gi, sem.at[PIECES])]
    for copy in copies:
        copy.start()
    for copy in copies:
        copy.wait()


def store(grad_input, grad_weight):
    anywhere = pl.BlockSpec(memory_space=pl.ANY)
    return pl.pallas_call(
        store_kernel,
        out_shape=(
            jax.ShapeDtypeStruct(grad_input.shape, BF16),
            jax.ShapeDtypeStruct(grad_weight.shape, BF16),
        ),
        in_specs=[anywhere] * 2,
        out_specs=(anywhere, anywhere),
        scratch_shapes=[pltpu.SemaphoreType.DMA((PIECES + 1,))],
        compiler_params=pltpu.CompilerParams(vmem_limit_bytes=2**20),
    )(grad_input, grad_weight)


def per_device_kernel(tokens, weight, grad_output):
    tl, il = tokens.shape
    ol = weight.shape[1]
    tb, ic = 4 * tl, il // (4 * CHUNKS)
    dma = pltpu.SemaphoreType.DMA
    code = pltpu.VMEM((3 * LAST, tb + GROUP, ic), BF16)
    code2 = pltpu.VMEM((6, tb + GROUP, ic // 2), BF16)
    anywhere = pl.BlockSpec(memory_space=pl.ANY)
    return store(*pl.pallas_call(
        kernel,
        out_shape=(
            jax.ShapeDtypeStruct(tokens.shape, BF16),
            jax.ShapeDtypeStruct(weight.shape, BF16),
        ),
        in_specs=[anywhere] * 3,
        out_specs=(anywhere, anywhere),
        scratch_shapes=[
            pltpu.VMEM((4 * tb, 4 * ol), BF16),
            pltpu.VMEM((2, tb // 2, ol), BF16),
            pltpu.VMEM((CHUNKS, 4 * tb, ic), BF16),
            pltpu.VMEM((ic, 4 * tb), BF16),
            pltpu.VMEM((CHUNKS, ic, 4 * ol), BF16),
            pltpu.VMEM((CHUNKS, 4 * tb, ic), F32),
            pltpu.VMEM((CHUNKS, ic, 4 * ol), BF16),
            pltpu.VMEM((CHUNKS, tb, ic), BF16),
            code, code, code, code, code2, code2, code2, code2,
            pltpu.VMEM((4 * tb, ic // 2), BF16), pltpu.SemaphoreType.REGULAR((3,)),
            dma((2,)), dma((4,)), dma((4,)), dma((4,)), dma((4,)), dma((CHUNKS + 1,)), dma((CHUNKS,)),
            dma((CHUNKS + 1, 4)), dma((3 * CHUNKS + 3,)), dma((3 * CHUNKS + 3,)), dma((2,)), dma((18,)),
        ],
        compiler_params=pltpu.CompilerParams(
            collective_id=0, has_side_effects=True, vmem_limit_bytes=46 * 2**20
        ),
    )(*[pltpu.with_memory_space_constraint(a, pltpu.HBM) for a in (tokens, weight, grad_output)]))


def solution(mesh):
    fours_fit = mesh.shape["row"] == 4 and mesh.shape["col"] == 4 and mesh.shape["depth"] == 2
    return jax.shard_map(
        per_device_kernel if fours_fit else per_device_general,
        mesh=mesh,
        in_specs=(
            P(("row", "col"), "depth"),
            P("depth", ("col", "row")),
            P("row", ("col", "depth")),
        ),
        out_specs=(P(("row", "col"), "depth"), P("depth", ("col", "row"))),
        check_vma=False,
    )
```
